128 devices in a mesh: batch: 1, seq_hi: 16 (over z, y), seq: 8 (over x, core).
Axes of the slice: x: 4, y: 4, z: 4, core: 2. Of those that a mesh axis runs over, the one named last changes fastest.
Arguments:
- x_seq: bfloat16 [32, 16384, 64], P('batch', ('seq_hi', 'seq'))
- w_f0: bfloat16 [3, 10, 64, 64], replicated
- w_f1: bfloat16 [3, 10, 64, 64], replicated
- w_g0: bfloat16 [3, 10, 64, 64], replicated
- w_g1: bfloat16 [3, 10, 64, 64], replicated
- w_res: bfloat16 [3, 10, 64, 64], replicated
- w_skip: bfloat16 [3, 10, 64, 64], replicated
Outputs:
- output 1: float32 [32, 16384, 64], P('batch', ('seq_hi', 'seq'))
- output 2: float32 [32, 16384, 64], P('batch', ('seq_hi', 'seq'))
All inputs are finite; a program needn't handle non-finite values.
Results may differ from the reference program's by a relative error of at most 0.0081759.
Values are sent between devices in bfloat16 or wider.
A program may use at most 1 GiB of HBM per device.

```python
import jax
import jax.numpy as jnp
from jax import lax

GROUP_SEQS = 32
SEQ_LEN = 16384
CHANNELS = 64
SKIP_CH = 64
DIL_CYCLE = 10
REPEATS = 3


def setup_inputs(seed: int = 0, part: int = 0) -> dict:
    keys = jax.random.split(jax.random.key(seed), 7)
    square = (REPEATS, DIL_CYCLE, CHANNELS, CHANNELS)
    tap_scale = (2 * CHANNELS) ** -0.5
    x_seq = jax.random.normal(jax.random.fold_in(keys[0], part), (GROUP_SEQS, SEQ_LEN, CHANNELS), jnp.float32)
    w_f0 = jax.random.normal(keys[1], square, jnp.float32) * tap_scale
    w_f1 = jax.random.normal(keys[2], square, jnp.float32) * tap_scale
    w_g0 = jax.random.normal(keys[3], square, jnp.float32) * tap_scale
    w_g1 = jax.random.normal(keys[4], square, jnp.float32) * tap_scale
    w_res = jax.random.normal(keys[5], square, jnp.float32) * (0.5 * CHANNELS ** -0.5)
    w_skip = jax.random.normal(keys[6], (REPEATS, DIL_CYCLE, CHANNELS, SKIP_CH), jnp.float32) * CHANNELS ** -0.5
    return {
        "x_seq": x_seq.astype(jnp.bfloat16),
        "w_f0": w_f0.astype(jnp.bfloat16),
        "w_f1": w_f1.astype(jnp.bfloat16),
        "w_g0": w_g0.astype(jnp.bfloat16),
        "w_g1": w_g1.astype(jnp.bfloat16),
        "w_res": w_res.astype(jnp.bfloat16),
        "w_skip": w_skip.astype(jnp.bfloat16),
    }


def mat_mul(left, right):
    return jnp.dot(left, right, preferred_element_type=jnp.float32)


def reference(x_seq, w_f0, w_f1, w_g0, w_g1, w_res, w_skip):
    def one_sequence(seq_in):
        residual = seq_in.astype(jnp.float32)
        skip_acc = jnp.zeros((SEQ_LEN, SKIP_CH), jnp.float32)
        for rep_idx in range(REPEATS):
            for cyc_idx in range(DIL_CYCLE):
                dilation = 2 ** cyc_idx
                current = residual.astype(jnp.bfloat16)
                delayed = jnp.pad(current[:SEQ_LEN - dilation], ((dilation, 0), (0, 0)))
                filter_pre = mat_mul(current, w_f1[rep_idx, cyc_idx]) + mat_mul(delayed, w_f0[rep_idx, cyc_idx])
                gate_pre = mat_mul(current, w_g1[rep_idx, cyc_idx]) + mat_mul(delayed, w_g0[rep_idx, cyc_idx])
                activated = (jnp.tanh(filter_pre) * jax.nn.sigmoid(gate_pre)).astype(jnp.bfloat16)
                residual = residual + mat_mul(activated, w_res[rep_idx, cyc_idx])
                skip_acc = skip_acc + mat_mul(activated, w_skip[rep_idx, cyc_idx])
        return residual, skip_acc
    h_out, skip_out = lax.map(one_sequence, x_seq)
    return h_out, skip_out
```

```python
import jax
import jax.numpy as jnp
from jax import lax
from jax.experimental import pallas as pl
from jax.experimental.pallas import tpu as pltpu
from jax.sharding import PartitionSpec as P

F32, BF = jnp.float32, jnp.bfloat16
SEQ_AXES = ("seq_hi", "seq")
NT = 8
HALO = 24
LAG1, LAG2 = 5, 4
CHANS, TILE, CYCLE = 64, 128, 10


def run_layers(reps, hs, ss, acts, us, hist, w1t, wrt, wst, lane):
    items = [(c, st, j) for c in range(CYCLE) for st in range(len(reps)) for j in range(0, NT, 2)]
    carry, gates, mixed, skips = {}, {}, {}, {}

    def front(t):
        c, st, j = items[t]
        d = 2**c
        nh = max(1, d // TILE)
        layer = reps[st] * CYCLE + c
        h, ub = hs[st], us[st]
        if j == 0:
            for i in range(4 - nh, 4):
                ub[i] = hist[layer, i]
            if d < TILE:
                carry[st] = pltpu.roll(ub[3], d, 1)
        u = [h[j].astype(BF), h[j + 1].astype(BF)]
        if d >= TILE:
            ub[4 + j], ub[5 + j] = u[0], u[1]
            q = d // TILE
            p = [ub[4 + j - q], ub[5 + j - q] if q > 1 else u[0]]
        else:
            r0, r1 = pltpu.roll(u[0], d, 1), pltpu.roll(u[1], d, 1)
            p = [jnp.where(lane < d, carry[st], r0), jnp.where(lane < d, r0, r1)]
            carry[st] = r1
        for i in range(2):
            k = j + i - (NT - 4)
            if k >= 4 - nh:
                hist[layer, k] = u[i]
        up = jnp.concatenate([jnp.concatenate(u, 1), jnp.concatenate(p, 1)], 0)
        gates[t] = jnp.dot(w1t[layer], up, preferred_element_type=F32)

    def middle(t):
        c, st, j = items[t]
        layer = reps[st] * CYCLE + c
        g = gates.pop(t)
        sig = jnp.tanh(g[CHANS:] * 0.5) * 0.5 + 0.5
        a = (jnp.tanh(g[:CHANS]) * sig).astype(BF)
        row = (c % 4) * CHANS
        cols = slice(j * TILE, (j + 2) * TILE)
        if c not in (3, 7, 9):
            acts[st][row : row + CHANS, cols] = a
        mixed[t] = jnp.dot(wrt[layer], a, preferred_element_type=F32)
        if c in (3, 7, 9):
            stack = jnp.concatenate([acts[st][:row, cols], a], 0)
            skips[t] = jnp.dot(wst[reps[st] * 3 + c // 4][:, : row + CHANS], stack, preferred_element_type=F32)

    def back(t):
        c, st, j = items[t]
        res = mixed.pop(t)
        h = hs[st]
        h[j] += res[:, :TILE]
        h[j + 1] += res[:, TILE:]
        if t in skips:
            res = skips.pop(t)
            ss[st][j] += res[:, :TILE]
            ss[st][j + 1] += res[:, TILE:]

    n = len(items)
    for t in range(n + LAG1 + LAG2):
        if t >= LAG1 + LAG2:
            back(t - LAG1 - LAG2)
        if t < n:
            front(t)
        if 0 <= t - LAG1 < n:
            middle(t - LAG1)


def kernel(x, w1t, wrt, wst, hout, sout, xbuf, hA, hB, hC, sA, sB, sC, aA, aB, aC, uA, uB, uC, hist, hstage, sstage,
           in_send, in_recv, halo_send, out_send, out_recv):
    hi, k = lax.axis_index("seq_hi"), lax.axis_index("seq")
    z, row = hi // 4, hi % 4
    me = row * 8 + k

    def device(zz, m):
        return {"seq_hi": zz * 4 + m // 8, "seq": m % 8}

    def own_copy(s):
        return pltpu.make_async_remote_copy(
            src_ref=x.at[s], dst_ref=xbuf.at[HALO + me], send_sem=in_send.at[s], recv_sem=in_recv.at[HALO + me],
            device_id=device(z, s), device_id_type=pl.DeviceIdType.MESH)

    def halo_copy(s):
        return pltpu.make_async_remote_copy(
            src_ref=x.at[s], dst_ref=xbuf.at[me - 8], send_sem=halo_send.at[s], recv_sem=in_recv.at[me - 8],
            device_id=device(z + 1, s), device_id_type=pl.DeviceIdType.MESH)

    def out_copy(i, src, dst, m):
        return pltpu.make_async_remote_copy(
            src_ref=src.at[m], dst_ref=dst.at[me], send_sem=out_send.at[i, m], recv_sem=out_recv.at[i, me],
            device_id=device(z, m), device_id_type=pl.DeviceIdType.MESH)

    sends_halo = jnp.logical_and(z < 3, row >= 1)

    @pl.when(sends_halo)
    def _():
        def start(o, c):
            halo_copy(lax.rem(me + o, 32)).start()
            return c
        lax.fori_loop(0, 32, start, 0)

    def start_own(o, c):
        own_copy(lax.rem(me + o, 32)).start()
        return c

    lax.fori_loop(1, 32, start_own, 0)

    lane = lax.broadcasted_iota(jnp.int32, (CHANS, TILE), 1)
    hist[...] = jnp.zeros_like(hist)
    xbuf[HALO + me] = x[me]

    @pl.when(z == 0)
    def _():
        xbuf[0:HALO] = jnp.zeros((HALO, CHANS, TILE), BF)

    def wait_tile(t):
        pltpu.make_async_copy(xbuf.at[t], xbuf.at[t], in_recv.at[t]).wait()

    @pl.when(z > 0)
    def _():
        def w(t, c):
            wait_tile(t)
            return c
        lax.fori_loop(0, HALO, w, 0)

    def macro(s):
        @pl.when(s >= 3)
        def _():
            hC[...] = hB[...]
            sC[...] = sB[...]

        @pl.when(s >= 2)
        def _():
            hB[...] = hA[...]
            sB[...] = sA[...]

        @pl.when(s == 0)
        def _():
            hA[...] = xbuf[0:8].astype(F32)
            hB[...] = xbuf[8:16].astype(F32)
            hC[...] = xbuf[16:24].astype(F32)
            for ref in (sA, sB, sC):
                ref[...] = jnp.zeros_like(ref)

        @pl.when(jnp.logical_and(s >= 1, s <= 4))
        def _():
            base = (s + 2) * NT

            def w(i, c):
                @pl.when(base + i != HALO + me)
                def _():
                    wait_tile(base + i)
                return c

            lax.fori_loop(0, NT, w, 0)
            hA[...] = xbuf[pl.ds(base, NT)].astype(F32)
            sA[...] = jnp.zeros_like(sA)

        reps = [0, jnp.minimum(s, 1), jnp.minimum(s, 2)]
        run_layers(reps, [hA, hB, hC], [sA, sB, sC], [aA, aB, aC], [uA, uB, uC], hist, w1t, wrt, wst, lane)

        @pl.when(s >= 3)
        def _():
            base = (s - 3) * NT
            hstage[pl.ds(base, NT)] = hC[...]
            sstage[pl.ds(base, NT)] = sC[...]

            def send(o, c):
                m = base + lax.rem(o + k, NT)

                @pl.when(m != me)
                def _():
                    out_copy(0, hstage, hout, m).start()
                    out_copy(1, sstage, sout, m).start()
                return c

            lax.fori_loop(0, NT, send, 0)

    lax.fori_loop(0, 7, lambda s, c: (macro(s), c)[1], 0)

    hout[me] = hstage[me]
    sout[me] = sstage[me]

    @pl.when(sends_halo)
    def _():
        def w(s, c):
            halo_copy(s).wait_send()
            return c
        lax.fori_loop(0, 32, w, 0)

    def drain(o, c):
        m = lax.rem(me + o, 32)
        own_copy(m).wait_send()
        out_copy(0, hstage, hout, m).wait_send()
        out_copy(1, sstage, sout, m).wait_send()
        pltpu.make_async_copy(hout.at[m], hout.at[m], out_recv.at[0, m]).wait()
        pltpu.make_async_copy(sout.at[m], sout.at[m], out_recv.at[1, m]).wait()
        return c

    lax.fori_loop(1, 32, drain, 0)


def solution(mesh):
    seq_spec = P("batch", SEQ_AXES, None)

    def local_stack(x_loc, w_f0, w_f1, w_g0, w_g1, w_res, w_skip):
        x_t = jnp.swapaxes(x_loc, 1, 2)
        flat = lambda w: jnp.swapaxes(w.reshape(30, CHANS, CHANS), 1, 2)
        w1t = jnp.concatenate([jnp.concatenate([flat(w_f1), flat(w_f0)], 2), jnp.concatenate([flat(w_g1), flat(w_g0)], 2)], 1)
        wrt = flat(w_res)
        ws = jnp.pad(jnp.swapaxes(w_skip, 2, 3), ((0, 0), (0, 2), (0, 0), (0, 0)))
        wst = ws.reshape(3, 3, 4, CHANS, CHANS).transpose(0, 1, 3, 2, 4).reshape(9, CHANS, 4 * CHANS)
        V, D = pltpu.VMEM, pltpu.SemaphoreType.DMA
        hid = (NT, CHANS, TILE)
        out = jax.ShapeDtypeStruct((32, CHANS, TILE), F32)
        h, skip = pl.pallas_call(
            kernel,
            out_shape=[out, out],
            in_specs=[pl.BlockSpec(memory_space=V)] * 4,
            out_specs=[pl.BlockSpec(memory_space=V)] * 2,
            scratch_shapes=[V((56, CHANS, TILE), BF)] + [V(hid, F32)] * 6 + [V((4 * CHANS, NT * TILE), BF)] * 3
            + [V((NT + 4, CHANS, TILE), BF)] * 3 + [V((30, 4, CHANS, TILE), BF)] + [V((32, CHANS, TILE), F32)] * 2
            + [D((32,)), D((56,)), D((32,)), D((2, 32)), D((2, 32))],
            compiler_params=pltpu.CompilerParams(vmem_limit_bytes=60 * 2**20, has_side_effects=True),
        )(x_t, w1t, wrt, wst)
        return jnp.swapaxes(h, 1, 2), jnp.swapaxes(skip, 1, 2)

    return jax.shard_map(local_stack, mesh=mesh, in_specs=(seq_spec, P(), P(), P(), P(), P(), P()), out_specs=(seq_spec, seq_spec), check_vma=False)
```

```python
import jax
import jax.numpy as jnp
from jax import lax
from jax.experimental import pallas as pl
from jax.experimental.pallas import tpu as pltpu
from jax.sharding import PartitionSpec as P

F32, BF = jnp.float32, jnp.bfloat16
SEQ_AXES = ("seq_hi", "seq")
MESH = pl.DeviceIdType.MESH
NT = 8
HALO = 24
LAG1, LAG2 = 5, 4
ZERO = 30
CHANS, TILE, CYCLE = 64, 128, 10


def run_layers(reps, resets, hs, ss, acts, us, hist, w1t, wrt, wst, lane):
    items = [(c, st, j) for c in range(CYCLE) for st in range(len(reps)) for j in range(0, NT, 2)]
    carry, gates, mixed, skips = {}, {}, {}, {}

    def front(t):
        c, st, j = items[t]
        d = 2**c
        nh = max(1, d // TILE)
        layer = reps[st] * CYCLE + c
        h, ub = hs[st], us[st]
        if j == 0:
            for i in range(4 - nh, 4):
                ub[i] = hist[jnp.where(resets[st], ZERO, layer), i]
            if d < TILE:
                carry[st] = pltpu.roll(ub[3], d, 1)
        u = [h[j].astype(BF), h[j + 1].astype(BF)]
        if d >= TILE:
            ub[4 + j], ub[5 + j] = u[0], u[1]
            q = d // TILE
            p = [ub[4 + j - q], ub[5 + j - q] if q > 1 else u[0]]
        else:
            r0, r1 = pltpu.roll(u[0], d, 1), pltpu.roll(u[1], d, 1)
            p = [jnp.where(lane < d, carry[st], r0), jnp.where(lane < d, r0, r1)]
            carry[st] = r1
        for i in range(2):
            k = j + i - (NT - 4)
            if k >= 4 - nh:
                hist[layer, k] = u[i]
        up = jnp.concatenate([jnp.concatenate(u, 1), jnp.concatenate(p, 1)], 0)
        gates[t] = jnp.dot(w1t[layer], up, preferred_element_type=F32)

    def middle(t):
        c, st, j = items[t]
        layer = reps[st] * CYCLE + c
        g = gates.pop(t)
        sig = jnp.tanh(g[CHANS:] * 0.5) * 0.5 + 0.5
        a = (jnp.tanh(g[:CHANS]) * sig).astype(BF)
        row = (c % 4) * CHANS
        cols = slice(j * TILE, (j + 2) * TILE)
        if c not in (3, 7, 9):
            acts[st][row : row + CHANS, cols] = a
        mixed[t] = jnp.dot(wrt[layer], a, preferred_element_type=F32)
        if c in (3, 7, 9):
            stack = jnp.concatenate([acts[st][:row, cols], a], 0)
            ws = jnp.concatenate([wst[layer - c % 4 + i] for i in range(c % 4 + 1)], 1)
            skips[t] = jnp.dot(ws, stack, preferred_element_type=F32)

    def back(t):
        c, st, j = items[t]
        res = mixed.pop(t)
        h = hs[st]
        h[j] += res[:, :TILE]
        h[j + 1] += res[:, TILE:]
        if t in skips:
            res = skips.pop(t)
            ss[st][j] += res[:, :TILE]
            ss[st][j + 1] += res[:, TILE:]

    n = len(items)
    for t in range(n + LAG1 + LAG2):
        if t >= LAG1 + LAG2:
            back(t - LAG1 - LAG2)
        if t < n:
            front(t)
        if 0 <= t - LAG1 < n:
            middle(t - LAG1)


def shift_of(s):
    return lax.rem((s % 8) // 2 + s % 2, 4)


def kernel(x_hbm, wf0, wf1, wg0, wg1, wres, wskip, hout, sout, x, w0, w1, w2, w3, w4, w5, w1t, wrt, wst, xbuf,
           hA, hB, hC, sA, sB, sC, aA, aB, aC, uA, uB, uC, hist, hstage, sstage,
           load_sem, in_send, in_recv, halo_send, out_send, out_recv):
    loads = [pltpu.make_async_copy(a, b, load_sem.at[i])
             for i, (a, b) in enumerate(zip((x_hbm, wf0, wf1, wg0, wg1, wres, wskip), (x, w0, w1, w2, w3, w4, w5)))]
    for load in loads:
        load.start()
    hi, k = lax.axis_index("seq_hi"), lax.axis_index("seq")
    z, row = hi // 4, hi % 4
    me = row * 8 + k
    first = 4 * z + shift_of(me)

    def device(h, m):
        return {"seq_hi": h, "seq": m}

    def place(s):
        e = lax.rem(hi - shift_of(s) + 16, 16)
        return e // 4, e % 4

    def own_copy(s):
        q, c = place(s)
        slot = (3 + c) * NT + k
        go = jnp.logical_or(q != z, s != me)
        return go, pltpu.make_async_remote_copy(
            src_ref=x.at[s], dst_ref=xbuf.at[slot], send_sem=in_send.at[s], recv_sem=in_recv.at[slot],
            device_id=device(q * 4 + s // 8, s % 8), device_id_type=MESH)

    def halo_copy(s):
        q, c = place(s)
        nxt = lax.rem(q + 1, 4)
        slot = lax.rem(c + 3, 4) * NT + k
        go = jnp.logical_and(c >= 1, jnp.logical_or(q != 3, hi < shift_of(s)))
        go = jnp.logical_and(go, jnp.logical_or(nxt != z, s != me))
        return go, pltpu.make_async_remote_copy(
            src_ref=x.at[s], dst_ref=xbuf.at[slot], send_sem=halo_send.at[s], recv_sem=in_recv.at[slot],
            device_id=device(nxt * 4 + s // 8, s % 8), device_id_type=MESH)

    def source(slot):
        g = first - 3 + slot // NT
        src = lax.rem(g + 16, 16)
        return g, src, jnp.logical_and(g >= 0, jnp.logical_or(src != hi, slot % NT != k))

    def out_copy(i, src, dst, t):
        g = lax.rem(first + t // NT, 16)
        return pltpu.make_async_remote_copy(
            src_ref=src.at[t], dst_ref=dst.at[me], send_sem=out_send.at[i, t], recv_sem=out_recv.at[i, me],
            device_id=device(g, t % NT), device_id_type=MESH)

    def out_goes(t):
        return jnp.logical_or(lax.rem(first + t // NT, 16) != hi, t % NT != k)

    def order(o):
        return lax.rem(me + 5 * o, 32)

    barrier = pltpu.get_barrier_semaphore()

    def greet(slot, c):
        g, src, remote = source(slot)

        @pl.when(remote)
        def _():
            pl.semaphore_signal(barrier, inc=1, device_id=device(src, slot % NT), device_id_type=MESH)
        return c

    lax.fori_loop(0, 56, greet, 0)
    peers = lax.fori_loop(0, 32, lambda s, n: n + own_copy(s)[0].astype(jnp.int32) + halo_copy(s)[0].astype(jnp.int32), jnp.int32(0))
    loads[0].wait()
    pl.semaphore_wait(barrier, peers)

    def start_halo(o, c):
        go, copy = halo_copy(order(o))
        pl.when(go)(copy.start)
        return c

    def start_own(o, c):
        go, copy = own_copy(order(o))
        pl.when(go)(copy.start)
        return c

    lax.fori_loop(0, 32, start_halo, 0)
    lax.fori_loop(0, 32, start_own, 0)

    for load in loads[1:]:
        load.wait()

    def prepare(c, carry):
        for r in range(3):
            layer = r * CYCLE + c
            top = jnp.concatenate([w1[r, c], w3[r, c]], 1)
            low = jnp.concatenate([w0[r, c], w2[r, c]], 1)
            w1t[layer] = jnp.concatenate([top, low], 0).astype(F32).T.astype(BF)
            last = jnp.concatenate([w4[r, c], w5[r, c]], 1).astype(F32).T.astype(BF)
            wrt[layer] = last[:CHANS]
            wst[layer] = last[CHANS:]
        return carry

    lax.fori_loop(0, CYCLE, prepare, 0)

    lane = lax.broadcasted_iota(jnp.int32, (CHANS, TILE), 1)
    hist[...] = jnp.zeros_like(hist)
    xbuf[(3 + row - shift_of(me)) * NT + k] = x[me]
    for kk in range(3):
        @pl.when(first - 3 + kk < 0)
        def _():
            xbuf[kk * NT : (kk + 1) * NT] = jnp.zeros((NT, CHANS, TILE), BF)

    def wait_slot(slot, c):
        @pl.when(source(slot)[2])
        def _():
            pltpu.make_async_copy(xbuf.at[slot], xbuf.at[slot], in_recv.at[slot]).wait()
        return c

    lax.fori_loop(0, 3 * NT, wait_slot, 0)

    def macro(s):
        @pl.when(s >= 3)
        def _():
            hC[...] = hB[...]
            sC[...] = sB[...]

        @pl.when(s >= 2)
        def _():
            hB[...] = hA[...]
            sB[...] = sA[...]

        @pl.when(s == 0)
        def _():
            hA[...] = xbuf[0:8].astype(F32)
            hB[...] = xbuf[8:16].astype(F32)
            hC[...] = xbuf[16:24].astype(F32)
            for ref in (sA, sB, sC):
                ref[...] = jnp.zeros_like(ref)

        @pl.when(jnp.logical_and(s >= 1, s <= 4))
        def _():
            base = (s + 2) * NT
            lax.fori_loop(base, base + NT, wait_slot, 0)
            hA[...] = xbuf[pl.ds(base, NT)].astype(F32)
            sA[...] = jnp.zeros_like(sA)

        reps = [0, jnp.minimum(s, 1), jnp.minimum(s, 2)]
        resets = [first - 3 + s + i == 16 for i in (2, 1, 0)]
        run_layers(reps, resets, [hA, hB, hC], [sA, sB, sC], [aA, aB, aC], [uA, uB, uC], hist, w1t, wrt, wst, lane)

        @pl.when(s >= 3)
        def _():
            base = (s - 3) * NT
            hstage[pl.ds(base, NT)] = hC[...]
            sstage[pl.ds(base, NT)] = sC[...]

            def send(o, c):
                t = base + lax.rem(3 * o + k, NT)

                @pl.when(out_goes(t))
                def _():
                    out_copy(0, hstage, hout, t).start()
                    out_copy(1, sstage, sout, t).start()
                return c

            lax.fori_loop(0, NT, send, 0)

    lax.fori_loop(0, 7, lambda s, c: (macro(s), c)[1], 0)

    keeps = row >= shift_of(me)

    @pl.when(keeps)
    def _():
        t = (row - shift_of(me)) * NT + k
        hout[me] = hstage[t]
        sout[me] = sstage[t]

    def drain(s, c):
        for go, copy in (own_copy(s), halo_copy(s)):
            pl.when(go)(copy.wait_send)

        @pl.when(out_goes(s))
        def _():
            out_copy(0, hstage, hout, s).wait_send()
            out_copy(1, sstage, sout, s).wait_send()

        @pl.when(own_copy(s)[0])
        def _():
            pltpu.make_async_copy(hout.at[s], hout.at[s], out_recv.at[0, s]).wait()
            pltpu.make_async_copy(sout.at[s], sout.at[s], out_recv.at[1, s]).wait()
        return c

    lax.fori_loop(0, 32, drain, 0)


def solution(mesh):
    seq_spec = P("batch", SEQ_AXES, None)

    def local_stack(x_loc, *weights):
        x_t = jnp.swapaxes(x_loc, 1, 2)
        V, D = pltpu.VMEM, pltpu.SemaphoreType.DMA
        hid = (NT, CHANS, TILE)
        out = jax.ShapeDtypeStruct((32, CHANS, TILE), F32)
        h, skip = pl.pallas_call(
            kernel,
            out_shape=[out, out],
            in_specs=[pl.BlockSpec(memory_space=pl.ANY)] * 7,
            out_specs=[pl.BlockSpec(memory_space=V)] * 2,
            scratch_shapes=[V((32, CHANS, TILE), BF)] + [V((3, CYCLE, CHANS, CHANS), BF)] * 6
            + [V((30, 2 * CHANS, 2 * CHANS), BF)] + [V((30, CHANS, CHANS), BF)] * 2
            + [V((56, CHANS, TILE), BF)] + [V(hid, F32)] * 6 + [V((4 * CHANS, NT * TILE), BF)] * 3
            + [V((NT + 4, CHANS, TILE), BF)] * 3 + [V((31, 4, CHANS, TILE), BF)] + [V((32, CHANS, TILE), F32)] * 2
            + [D((7,)), D((32,)), D((56,)), D((32,)), D((2, 32)), D((2, 32))],
            compiler_params=pltpu.CompilerParams(vmem_limit_bytes=60 * 2**20, has_side_effects=True, collective_id=0),
        )(x_t, *weights)
        return jnp.swapaxes(h, 1, 2), jnp.swapaxes(skip, 1, 2)

    return jax.shard_map(local_stack, mesh=mesh, in_specs=(seq_spec, P(), P(), P(), P(), P(), P()), out_specs=(seq_spec, seq_spec), check_vma=False)
```

```python
import jax
import jax.numpy as jnp
from jax import lax
from jax.experimental import pallas as pl
from jax.experimental.pallas import tpu as pltpu
from jax.sharding import PartitionSpec as P

F32, BF = jnp.float32, jnp.bfloat16
SEQ_AXES = ("seq_hi", "seq")
MESH = pl.DeviceIdType.MESH
NT = 8
HALO = 24
LAG1, LAG2 = 5, 4
ZERO = 30
CHANS, TILE, CYCLE = 64, 128, 10


def run_layers(reps, resets, hs, ss, acts, us, hist, w1t, wrt, wst, lane):
    items = [(c, st, j) for c in range(CYCLE) for st in range(len(reps)) for j in range(0, NT, 2)]
    carry, gates, mixed, skips = {}, {}, {}, {}

    def front(t):
        c, st, j = items[t]
        d = 2**c
        nh = max(1, d // TILE)
        layer = reps[st] * CYCLE + c
        h, ub = hs[st], us[st]
        if j == 0:
            for i in range(4 - nh, 4):
                ub[i] = hist[jnp.where(resets[st], ZERO, layer), i]
            if d < TILE:
                carry[st] = pltpu.roll(ub[3], d, 1)
        u = [h[j].astype(BF), h[j + 1].astype(BF)]
        if d >= TILE:
            ub[4 + j], ub[5 + j] = u[0], u[1]
            q = d // TILE
            p = [ub[4 + j - q], ub[5 + j - q] if q > 1 else u[0]]
        else:
            r0, r1 = pltpu.roll(u[0], d, 1), pltpu.roll(u[1], d, 1)
            p = [jnp.where(lane < d, carry[st], r0), jnp.where(lane < d, r0, r1)]
            carry[st] = r1
        for i in range(2):
            k = j + i - (NT - 4)
            if k >= 4 - nh:
                hist[layer, k] = u[i]
        up = jnp.concatenate([jnp.concatenate(u, 1), jnp.concatenate(p, 1)], 0)
        gates[t] = jnp.dot(w1t[layer], up, preferred_element_type=F32)

    def middle(t):
        c, st, j = items[t]
        layer = reps[st] * CYCLE + c
        g = gates.pop(t)
        sig = jnp.tanh(g[CHANS:] * 0.5) * 0.5 + 0.5
        a = (jnp.tanh(g[:CHANS]) * sig).astype(BF)
        row = (c % 4) * CHANS
        cols = slice(j * TILE, (j + 2) * TILE)
        if c not in (3, 7, 9):
            acts[st][row : row + CHANS, cols] = a
        mixed[t] = jnp.dot(wrt[layer], a, preferred_element_type=F32)
        if c in (3, 7, 9):
            stack = jnp.concatenate([acts[st][:row, cols], a], 0)
            ws = jnp.concatenate([wst[layer - c % 4 + i] for i in range(c % 4 + 1)], 1)
            skips[t] = jnp.dot(ws, stack, preferred_element_type=F32)

    def back(t):
        c, st, j = items[t]
        res = mixed.pop(t)
        h = hs[st]
        h[j] += res[:, :TILE]
        h[j + 1] += res[:, TILE:]
        if t in skips:
            res = skips.pop(t)
            ss[st][j] += res[:, :TILE]
            ss[st][j + 1] += res[:, TILE:]

    n = len(items)
    for t in range(n + LAG1 + LAG2):
        if t >= LAG1 + LAG2:
            back(t - LAG1 - LAG2)
        if t < n:
            front(t)
        if 0 <= t - LAG1 < n:
            middle(t - LAG1)


def low(v, n):
    return lax.bitwise_and(v, jnp.int32(n - 1))


def high(v, bits):
    return lax.shift_right_logical(v, jnp.int32(bits))


def shift_of(k):
    return low(high(k, 1) + low(k, 2), 4)


def kernel(x_hbm, wf0, wf1, wg0, wg1, wres, wskip, hout, sout, x, w0, w1, w2, w3, w4, w5, w1t, wrt, wst, xbuf,
           hA, hB, hC, sA, sB, sC, aA, aB, aC, uA, uB, uC, hist, hstage, sstage,
           load_sem, in_send, in_recv, halo_send, out_send, out_recv):
    loads = [pltpu.make_async_copy(a, b, load_sem.at[i])
             for i, (a, b) in enumerate(zip((x_hbm, wf0, wf1, wg0, wg1, wres, wskip), (x, w0, w1, w2, w3, w4, w5)))]
    for load in loads:
        load.start()
    hi, k = lax.axis_index("seq_hi"), lax.axis_index("seq")
    z, row = high(hi, 2), low(hi, 4)
    me = row * 8 + k
    shift = shift_of(k)
    first = 4 * z + shift
    mine = (3 + row - shift) * NT + k
    keeps = row >= shift

    def device(h, m):
        return {"seq_hi": h, "seq": m}

    def place(s):
        off = shift_of(low(s, 8))
        e = low(hi - off, 16)
        q, c = high(e, 2), low(e, 4)
        return q, c, jnp.logical_and(c >= 1, jnp.logical_or(q != 3, hi < off))

    def own_copy(s):
        q, c, _ = place(s)
        slot = (3 + c) * NT + k
        return pltpu.make_async_remote_copy(
            src_ref=x.at[s], dst_ref=xbuf.at[slot], send_sem=in_send.at[s], recv_sem=in_recv.at[slot],
            device_id=device(q * 4 + high(s, 3), low(s, 8)), device_id_type=MESH)

    def owns(s):
        return jnp.logical_or(s != me, jnp.logical_not(keeps))

    def halo_copy(s):
        q, c, _ = place(s)
        slot = (c - 1) * NT + k
        return pltpu.make_async_remote_copy(
            src_ref=x.at[s], dst_ref=xbuf.at[slot], send_sem=halo_send.at[s], recv_sem=in_recv.at[slot],
            device_id=device(low(q + 1, 4) * 4 + high(s, 3), low(s, 8)), device_id_type=MESH)

    def halos(s):
        return jnp.logical_and(place(s)[2], jnp.logical_or(s != me, keeps))

    def out_copy(i, src, dst, t):
        g = low(first + high(t, 3), 16)
        return pltpu.make_async_remote_copy(
            src_ref=src.at[t], dst_ref=dst.at[me], send_sem=out_send.at[i, t], recv_sem=out_recv.at[i, me],
            device_id=device(g, low(t, NT)), device_id_type=MESH)

    def leaves(t):
        return t + 3 * NT != mine

    def order(o):
        return low(me + 7 * o, 32)

    barrier = pltpu.get_barrier_semaphore()

    def greet(i, c):
        for kk in range(7):
            g = first - 3 + kk

            @pl.when(jnp.logical_and(g >= 0, kk * NT + i != mine))
            def _():
                pl.semaphore_signal(barrier, inc=1, device_id=device(low(g, 16), i), device_id_type=MESH)
        return c

    lax.fori_loop(0, NT, greet, 0)
    peers = jnp.int32(31)
    for m in range(NT):
        peers = peers + 4 * place(jnp.int32(m))[2].astype(jnp.int32)
    loads[0].wait()
    pl.semaphore_wait(barrier, peers)

    def start_halo(o, c):
        s = order(o)

        @pl.when(halos(s))
        def _():
            halo_copy(s).start()
        return c

    def start_own(o, c):
        s = order(o)

        @pl.when(owns(s))
        def _():
            own_copy(s).start()
        return c

    lax.fori_loop(0, 32, start_halo, 0)
    lax.fori_loop(0, 32, start_own, 0)

    for load in loads[1:]:
        load.wait()

    def prepare(c, carry):
        for r in range(3):
            layer = r * CYCLE + c
            top = jnp.concatenate([w1[r, c], w3[r, c]], 1)
            bottom = jnp.concatenate([w0[r, c], w2[r, c]], 1)
            w1t[layer] = jnp.concatenate([top, bottom], 0).astype(F32).T.astype(BF)
            last = jnp.concatenate([w4[r, c], w5[r, c]], 1).astype(F32).T.astype(BF)
            wrt[layer] = last[:CHANS]
            wst[layer] = last[CHANS:]
        return carry

    lax.fori_loop(0, CYCLE, prepare, 0)

    lane = lax.broadcasted_iota(jnp.int32, (CHANS, TILE), 1)
    hist[...] = jnp.zeros_like(hist)
    xbuf[mine] = x[me]
    for kk in range(3):
        @pl.when(first - 3 + kk < 0)
        def _():
            xbuf[kk * NT : (kk + 1) * NT] = jnp.zeros((NT, CHANS, TILE), BF)

    def wait_chunk(kk):
        @pl.when(first - 3 + kk >= 0)
        def _():
            def wait_slot(slot, c):
                @pl.when(slot != mine)
                def _():
                    pltpu.make_async_copy(xbuf.at[slot], xbuf.at[slot], in_recv.at[slot]).wait()
                return c

            lax.fori_loop(kk * NT, kk * NT + NT, wait_slot, 0)

    for kk in range(3):
        wait_chunk(kk)

    def macro(s):
        @pl.when(s >= 3)
        def _():
            hC[...] = hB[...]
            sC[...] = sB[...]

        @pl.when(s >= 2)
        def _():
            hB[...] = hA[...]
            sB[...] = sA[...]

        @pl.when(s == 0)
        def _():
            hA[...] = xbuf[0:8].astype(F32)
            hB[...] = xbuf[8:16].astype(F32)
            hC[...] = xbuf[16:24].astype(F32)
            for ref in (sA, sB, sC):
                ref[...] = jnp.zeros_like(ref)

        @pl.when(jnp.logical_and(s >= 1, s <= 4))
        def _():
            wait_chunk(s + 2)
            hA[...] = xbuf[pl.ds((s + 2) * NT, NT)].astype(F32)
            sA[...] = jnp.zeros_like(sA)

        reps = [0, jnp.minimum(s, 1), jnp.minimum(s, 2)]
        resets = [first - 3 + s + i == 16 for i in (2, 1, 0)]
        run_layers(reps, resets, [hA, hB, hC], [sA, sB, sC], [aA, aB, aC], [uA, uB, uC], hist, w1t, wrt, wst, lane)

        @pl.when(s >= 3)
        def _():
            base = (s - 3) * NT
            hstage[pl.ds(base, NT)] = hC[...]
            sstage[pl.ds(base, NT)] = sC[...]

            def send(o, c):
                t = base + low(3 * o + k, NT)

                @pl.when(leaves(t))
                def _():
                    out_copy(0, hstage, hout, t).start()
                    out_copy(1, sstage, sout, t).start()
                return c

            lax.fori_loop(0, NT, send, 0)

    lax.fori_loop(0, 7, lambda s, c: (macro(s), c)[1], 0)

    @pl.when(keeps)
    def _():
        hout[me] = hstage[mine - 3 * NT]
        sout[me] = sstage[mine - 3 * NT]

    def drain_sends(s, c):
        @pl.when(owns(s))
        def _():
            own_copy(s).wait_send()

        @pl.when(halos(s))
        def _():
            halo_copy(s).wait_send()

        @pl.when(leaves(s))
        def _():
            out_copy(0, hstage, hout, s).wait_send()
            out_copy(1, sstage, sout, s).wait_send()
        return c

    lax.fori_loop(0, 32, drain_sends, 0)

    def drain(s, c):
        @pl.when(owns(s))
        def _():
            pltpu.make_async_copy(hout.at[s], hout.at[s], out_recv.at[0, s]).wait()
            pltpu.make_async_copy(sout.at[s], sout.at[s], out_recv.at[1, s]).wait()
        return c

    lax.fori_loop(0, 32, drain, 0)


def solution(mesh):
    seq_spec = P("batch", SEQ_AXES, None)

    def local_stack(x_loc, *weights):
        x_t = jnp.swapaxes(x_loc, 1, 2)
        V, D = pltpu.VMEM, pltpu.SemaphoreType.DMA
        hid = (NT, CHANS, TILE)
        out = jax.ShapeDtypeStruct((32, CHANS, TILE), F32)
        h, skip = pl.pallas_call(
            kernel,
            out_shape=[out, out],
            in_specs=[pl.BlockSpec(memory_space=pltpu.HBM)] * 7,
            out_specs=[pl.BlockSpec(memory_space=V)] * 2,
            scratch_shapes=[V((32, CHANS, TILE), BF)] + [V((3, CYCLE, CHANS, CHANS), BF)] * 6
            + [V((30, 2 * CHANS, 2 * CHANS), BF)] + [V((30, CHANS, CHANS), BF)] * 2
            + [V((56, CHANS, TILE), BF)] + [V(hid, F32)] * 6 + [V((4 * CHANS, NT * TILE), BF)] * 3
            + [V((NT + 4, CHANS, TILE), BF)] * 3 + [V((31, 4, CHANS, TILE), BF)] + [V((32, CHANS, TILE), F32)] * 2
            + [D((7,)), D((32,)), D((56,)), D((32,)), D((2, 32)), D((2, 32))],
            compiler_params=pltpu.CompilerParams(vmem_limit_bytes=24 * 2**20, has_side_effects=True, collective_id=0),
        )(*[pltpu.with_memory_space_constraint(a, pltpu.HBM) for a in (x_t, *weights)])
        return jnp.swapaxes(h, 1, 2), jnp.swapaxes(skip, 1, 2)

    return jax.shard_map(local_stack, mesh=mesh, in_specs=(seq_spec, P(), P(), P(), P(), P(), P()), out_specs=(seq_spec, seq_spec), check_vma=False)
```

```python
import jax
import jax.numpy as jnp
from jax import lax
from jax.experimental import pallas as pl
from jax.experimental.pallas import tpu as pltpu
from jax.sharding import PartitionSpec as P

F32, BF = jnp.float32, jnp.bfloat16
SEQ_AXES = ("seq_hi", "seq")
MESH = pl.DeviceIdType.MESH
NT = 8
HALO = 24
LAG1, LAG2 = 5, 4
ZERO = 30
CHANS, TILE, CYCLE = 64, 128, 10


def run_layers(reps, resets, hs, ss, acts, us, hist, w1t, wrt, wst, lane):
    items = [(c, st, j) for c in range(CYCLE) for st in range(len(reps)) for j in range(0, NT, 2)]
    carry, gates, mixed, skips = {}, {}, {}, {}

    def front(t):
        c, st, j = items[t]
        d = 2**c
        nh = max(1, d // TILE)
        layer = reps[st] * CYCLE + c
        h, ub = hs[st], us[st]
        if j == 0:
            for i in range(4 - nh, 4):
                ub[i] = hist[jnp.where(resets[st], ZERO, layer), i]
            if d < TILE:
                carry[st] = pltpu.roll(ub[3], d, 1)
        u = [h[j].astype(BF), h[j + 1].astype(BF)]
        if d >= TILE:
            ub[4 + j], ub[5 + j] = u[0], u[1]
            q = d // TILE
            p = [ub[4 + j - q], ub[5 + j - q] if q > 1 else u[0]]
        else:
            r0, r1 = pltpu.roll(u[0], d, 1), pltpu.roll(u[1], d, 1)
            p = [jnp.where(lane < d, carry[st], r0), jnp.where(lane < d, r0, r1)]
            carry[st] = r1
        for i in range(2):
            k = j + i - (NT - 4)
            if k >= 4 - nh:
                hist[layer, k] = u[i]
        up = jnp.concatenate([jnp.concatenate(u, 1), jnp.concatenate(p, 1)], 0)
        gates[t] = jnp.dot(w1t[layer], up, preferred_element_type=F32)

    def middle(t):
        c, st, j = items[t]
        layer = reps[st] * CYCLE + c
        g = gates.pop(t)
        sig = jnp.tanh(g[CHANS:] * 0.5) * 0.5 + 0.5
        a = (jnp.tanh(g[:CHANS]) * sig).astype(BF)
        row = (c % 4) * CHANS
        cols = slice(j * TILE, (j + 2) * TILE)
        if c not in (3, 7, 9):
            acts[st][row : row + CHANS, cols] = a
        mixed[t] = jnp.dot(wrt[layer], a, preferred_element_type=F32)
        if c in (3, 7, 9):
            stack = jnp.concatenate([acts[st][:row, cols], a], 0)
            ws = jnp.concatenate([wst[layer - c % 4 + i] for i in range(c % 4 + 1)], 1)
            skips[t] = jnp.dot(ws, stack, preferred_element_type=F32)

    def back(t):
        c, st, j = items[t]
        res = mixed.pop(t)
        h = hs[st]
        h[j] += res[:, :TILE]
        h[j + 1] += res[:, TILE:]
        if t in skips:
            res = skips.pop(t)
            ss[st][j] += res[:, :TILE]
            ss[st][j + 1] += res[:, TILE:]

    n = len(items)
    for t in range(n + LAG1 + LAG2):
        if t >= LAG1 + LAG2:
            back(t - LAG1 - LAG2)
        if t < n:
            front(t)
        if 0 <= t - LAG1 < n:
            middle(t - LAG1)


def low(v, n):
    return lax.bitwise_and(v, jnp.int32(n - 1))


def high(v, bits):
    return lax.shift_right_logical(v, jnp.int32(bits))


def shift_of(s):
    r, x, core = high(s, 3), high(low(s, 8), 1), low(s, 2)
    return low(x + r + 2 * core, 4) - 1 - low(r, 2)


def kernel(x_hbm, wf0, wf1, wg0, wg1, wres, wskip, hout, sout, x, w0, w1, w2, w3, w4, w5, w1t, wrt, wst, xbuf,
           hA, hB, hC, sA, sB, sC, aA, aB, aC, uA, uB, uC, hist, hstage, sstage,
           load_sem, in_send, in_recv, halo_send, out_send, out_recv):
    loads = [pltpu.make_async_copy(a, b, load_sem.at[i])
             for i, (a, b) in enumerate(zip((x_hbm, wf0, wf1, wg0, wg1, wres, wskip), (x, w0, w1, w2, w3, w4, w5)))]
    for load in loads:
        load.start()
    hi, k = lax.axis_index("seq_hi"), lax.axis_index("seq")
    z, row = high(hi, 2), low(hi, 4)
    me = row * 8 + k
    first = low(4 * z + shift_of(me), 16)

    def device(h, m):
        return {"seq_hi": h, "seq": m}

    def place(s):
        return dealt(shift_of(s))

    def dealt(off):
        e = low(hi - off, 16)
        q, c = high(e, 2), low(e, 4)
        return q, c, jnp.logical_and(c >= 1, low(4 * q + 4 + off, 16) + c >= 4)

    my_q, my_c, my_halo = place(me)
    keeps = my_q == z
    reuses = jnp.logical_and(my_halo, low(my_q + 1, 4) == z)
    mine = jnp.where(keeps, (3 + my_c) * NT + k, jnp.where(reuses, (my_c - 1) * NT + k, -1))

    def own_copy(s):
        q, c, _ = place(s)
        slot = (3 + c) * NT + k
        return pltpu.make_async_remote_copy(
            src_ref=x.at[s], dst_ref=xbuf.at[slot], send_sem=in_send.at[s], recv_sem=in_recv.at[slot],
            device_id=device(q * 4 + high(s, 3), low(s, 8)), device_id_type=MESH)

    def owns(s):
        return jnp.logical_or(s != me, jnp.logical_not(keeps))

    def halo_copy(s):
        q, c, _ = place(s)
        slot = (c - 1) * NT + k
        return pltpu.make_async_remote_copy(
            src_ref=x.at[s], dst_ref=xbuf.at[slot], send_sem=halo_send.at[s], recv_sem=in_recv.at[slot],
            device_id=device(low(q + 1, 4) * 4 + high(s, 3), low(s, 8)), device_id_type=MESH)

    def halos(s):
        return jnp.logical_and(place(s)[2], jnp.logical_or(s != me, jnp.logical_not(reuses)))

    def out_copy(i, src, dst, t):
        g = low(first + high(t, 3), 16)
        return pltpu.make_async_remote_copy(
            src_ref=src.at[t], dst_ref=dst.at[me], send_sem=out_send.at[i, t], recv_sem=out_recv.at[i, me],
            device_id=device(g, low(t, NT)), device_id_type=MESH)

    def leaves(t):
        return t + 3 * NT != mine

    barrier = pltpu.get_barrier_semaphore()

    def greet(i, c):
        for kk in range(7):
            g = first - 3 + kk

            @pl.when(jnp.logical_and(g >= 0, kk * NT + i != mine))
            def _():
                pl.semaphore_signal(barrier, inc=1, device_id=device(low(g, 16), i), device_id_type=MESH)
        return c

    lax.fori_loop(0, NT, greet, 0)
    peers = 32 - keeps.astype(jnp.int32) - reuses.astype(jnp.int32)
    for m in range(4):
        for parity in range(2):
            peers = peers + 4 * dealt(jnp.int32(m - 1 - parity))[2].astype(jnp.int32)
    loads[0].wait()
    pl.semaphore_wait(barrier, peers)

    def spread(body):
        core = low(k, 2)
        start = row + high(k, 1) + 2 * core

        def turn(i, carry):
            m = low(start + i, 4)
            for parity in range(2):
                q, c, halo = dealt(m - 1 - low(row + parity, 2))
                for j in range(4):
                    r, co = low(row + parity + 2 * (j // 2), 4), low(core + j, 2)
                    s = r * 8 + 2 * low(m - r - 2 * co, 4) + co
                    body(s, q, c, halo, r)
            return carry

        lax.fori_loop(0, 4, turn, 0)

    def start_halo(s, q, c, halo, r):
        @pl.when(jnp.logical_and(halo, jnp.logical_or(s != me, jnp.logical_not(reuses))))
        def _():
            slot = (c - 1) * NT + k
            pltpu.make_async_remote_copy(
                src_ref=x.at[s], dst_ref=xbuf.at[slot], send_sem=halo_send.at[s], recv_sem=in_recv.at[slot],
                device_id=device(low(q + 1, 4) * 4 + r, low(s, 8)), device_id_type=MESH).start()

    def start_own(s, q, c, halo, r):
        @pl.when(owns(s))
        def _():
            slot = (3 + c) * NT + k
            pltpu.make_async_remote_copy(
                src_ref=x.at[s], dst_ref=xbuf.at[slot], send_sem=in_send.at[s], recv_sem=in_recv.at[slot],
                device_id=device(q * 4 + r, low(s, 8)), device_id_type=MESH).start()

    spread(start_halo)
    spread(start_own)

    for load in loads[1:]:
        load.wait()

    def prepare(c, carry):
        for r in range(3):
            layer = r * CYCLE + c
            top = jnp.concatenate([w1[r, c], w3[r, c]], 1)
            bottom = jnp.concatenate([w0[r, c], w2[r, c]], 1)
            w1t[layer] = jnp.concatenate([top, bottom], 0).astype(F32).T.astype(BF)
            last = jnp.concatenate([w4[r, c], w5[r, c]], 1).astype(F32).T.astype(BF)
            wrt[layer] = last[:CHANS]
            wst[layer] = last[CHANS:]
        return carry

    lax.fori_loop(0, CYCLE, prepare, 0)

    lane = lax.broadcasted_iota(jnp.int32, (CHANS, TILE), 1)
    hist[...] = jnp.zeros_like(hist)

    @pl.when(mine >= 0)
    def _():
        xbuf[jnp.maximum(mine, 0)] = x[me]

    for kk in range(3):
        @pl.when(first - 3 + kk < 0)
        def _():
            xbuf[kk * NT : (kk + 1) * NT] = jnp.zeros((NT, CHANS, TILE), BF)

    def wait_chunk(kk):
        @pl.when(first - 3 + kk >= 0)
        def _():
            def wait_slot(slot, c):
                @pl.when(slot != mine)
                def _():
                    pltpu.make_async_copy(xbuf.at[slot], xbuf.at[slot], in_recv.at[slot]).wait()
                return c

            lax.fori_loop(kk * NT, kk * NT + NT, wait_slot, 0)

    for kk in range(3):
        wait_chunk(kk)

    def macro(s):
        @pl.when(s >= 3)
        def _():
            hC[...] = hB[...]
            sC[...] = sB[...]

        @pl.when(s >= 2)
        def _():
            hB[...] = hA[...]
            sB[...] = sA[...]

        @pl.when(s == 0)
        def _():
            hA[...] = xbuf[0:8].astype(F32)
            hB[...] = xbuf[8:16].astype(F32)
            hC[...] = xbuf[16:24].astype(F32)
            for ref in (sA, sB, sC):
                ref[...] = jnp.zeros_like(ref)

        @pl.when(jnp.logical_and(s >= 1, s <= 4))
        def _():
            wait_chunk(s + 2)
            hA[...] = xbuf[pl.ds((s + 2) * NT, NT)].astype(F32)
            sA[...] = jnp.zeros_like(sA)

        reps = [0, jnp.minimum(s, 1), jnp.minimum(s, 2)]
        resets = [first - 3 + s + i == 16 for i in (2, 1, 0)]
        run_layers(reps, resets, [hA, hB, hC], [sA, sB, sC], [aA, aB, aC], [uA, uB, uC], hist, w1t, wrt, wst, lane)

        @pl.when(s >= 3)
        def _():
            base = (s - 3) * NT
            hstage[pl.ds(base, NT)] = hC[...]
            sstage[pl.ds(base, NT)] = sC[...]

            def send(o, c):
                t = base + low(3 * o + k, NT)

                @pl.when(leaves(t))
                def _():
                    out_copy(0, hstage, hout, t).start()
                    out_copy(1, sstage, sout, t).start()
                return c

            lax.fori_loop(0, NT, send, 0)

    lax.fori_loop(0, 7, lambda s, c: (macro(s), c)[1], 0)

    @pl.when(keeps)
    def _():
        hout[me] = hstage[jnp.maximum(mine - 3 * NT, 0)]
        sout[me] = sstage[jnp.maximum(mine - 3 * NT, 0)]

    def drain_sends(s, c):
        @pl.when(owns(s))
        def _():
            own_copy(s).wait_send()

        @pl.when(halos(s))
        def _():
            halo_copy(s).wait_send()

        @pl.when(leaves(s))
        def _():
            out_copy(0, hstage, hout, s).wait_send()
            out_copy(1, sstage, sout, s).wait_send()
        return c

    lax.fori_loop(0, 32, drain_sends, 0)

    def drain(s, c):
        @pl.when(owns(s))
        def _():
            pltpu.make_async_copy(hout.at[s], hout.at[s], out_recv.at[0, s]).wait()
            pltpu.make_async_copy(sout.at[s], sout.at[s], out_recv.at[1, s]).wait()
        return c

    lax.fori_loop(0, 32, drain, 0)


def solution(mesh):
    seq_spec = P("batch", SEQ_AXES, None)

    def local_stack(x_loc, *weights):
        x_t = jnp.swapaxes(x_loc, 1, 2)
        V, D = pltpu.VMEM, pltpu.SemaphoreType.DMA
        hid = (NT, CHANS, TILE)
        out = jax.ShapeDtypeStruct((32, CHANS, TILE), F32)
        h, skip = pl.pallas_call(
            kernel,
            out_shape=[out, out],
            in_specs=[pl.BlockSpec(memory_space=pltpu.HBM)] * 7,
            out_specs=[pl.BlockSpec(memory_space=V)] * 2,
            scratch_shapes=[V((32, CHANS, TILE), BF)] + [V((3, CYCLE, CHANS, CHANS), BF)] * 6
            + [V((30, 2 * CHANS, 2 * CHANS), BF)] + [V((30, CHANS, CHANS), BF)] * 2
            + [V((56, CHANS, TILE), BF)] + [V(hid, F32)] * 6 + [V((4 * CHANS, NT * TILE), BF)] * 3
            + [V((NT + 4, CHANS, TILE), BF)] * 3 + [V((31, 4, CHANS, TILE), BF)] + [V((32, CHANS, TILE), F32)] * 2
            + [D((7,)), D((32,)), D((56,)), D((32,)), D((2, 32)), D((2, 32))],
            compiler_params=pltpu.CompilerParams(vmem_limit_bytes=24 * 2**20, has_side_effects=True, collective_id=0),
        )(*[pltpu.with_memory_space_constraint(a, pltpu.HBM) for a in (x_t, *weights)])
        return jnp.swapaxes(h, 1, 2), jnp.swapaxes(skip, 1, 2)

    return jax.shard_map(local_stack, mesh=mesh, in_specs=(seq_spec, P(), P(), P(), P(), P(), P()), out_specs=(seq_spec, seq_spec), check_vma=False)
```

```python
import jax
import jax.numpy as jnp
from jax import lax
from jax.experimental import pallas as pl
from jax.experimental.pallas import tpu as pltpu
from jax.sharding import PartitionSpec as P

F32, BF = jnp.float32, jnp.bfloat16
SEQ_AXES = ("seq_hi", "seq")
MESH = pl.DeviceIdType.MESH
NT = 8
HALO = 24
LAG1, LAG2 = 5, 4
ZERO = 30
CHANS, TILE, CYCLE = 64, 128, 10


def run_layers(reps, resets, hs, ss, acts, us, hist, w1t, wrt, wst, lane):
    items = [(c, st, j) for c in range(CYCLE) for st in range(len(reps)) for j in range(0, NT, 2)]
    carry, gates, mixed, skips = {}, {}, {}, {}

    def front(t):
        c, st, j = items[t]
        d = 2**c
        nh = max(1, d // TILE)
        layer = reps[st] * CYCLE + c
        h, ub = hs[st], us[st]
        if j == 0:
            for i in range(4 - nh, 4):
                ub[i] = hist[jnp.where(resets[st], ZERO, layer), i]
            if d < TILE:
                carry[st] = pltpu.roll(ub[3], d, 1)
        u = [h[j].astype(BF), h[j + 1].astype(BF)]
        if d >= TILE:
            ub[4 + j], ub[5 + j] = u[0], u[1]
            q = d // TILE
            p = [ub[4 + j - q], ub[5 + j - q] if q > 1 else u[0]]
        else:
            r0, r1 = pltpu.roll(u[0], d, 1), pltpu.roll(u[1], d, 1)
            p = [jnp.where(lane < d, carry[st], r0), jnp.where(lane < d, r0, r1)]
            carry[st] = r1
        for i in range(2):
            k = j + i - (NT - 4)
            if k >= 4 - nh:
                hist[layer, k] = u[i]
        up = jnp.concatenate([jnp.concatenate(u, 1), jnp.concatenate(p, 1)], 0)
        gates[t] = jnp.dot(w1t[layer], up, preferred_element_type=F32)

    def middle(t):
        c, st, j = items[t]
        layer = reps[st] * CYCLE + c
        g = gates.pop(t)
        sig = jnp.tanh(g[CHANS:] * 0.5) * 0.5 + 0.5
        a = (jnp.tanh(g[:CHANS]) * sig).astype(BF)
        row = (c % 4) * CHANS
        cols = slice(j * TILE, (j + 2) * TILE)
        if c not in (3, 7, 9):
            acts[st][row : row + CHANS, cols] = a
        mixed[t] = jnp.dot(wrt[layer], a, preferred_element_type=F32)
        if c in (3, 7, 9):
            stack = jnp.concatenate([acts[st][:row, cols], a], 0)
            ws = jnp.concatenate([wst[layer - c % 4 + i] for i in range(c % 4 + 1)], 1)
            skips[t] = jnp.dot(ws, stack, preferred_element_type=F32)

    def back(t):
        c, st, j = items[t]
        res = mixed.pop(t)
        h = hs[st]
        h[j] += res[:, :TILE]
        h[j + 1] += res[:, TILE:]
        if t in skips:
            res = skips.pop(t)
            ss[st][j] += res[:, :TILE]
            ss[st][j + 1] += res[:, TILE:]

    n = len(items)
    for t in range(n + LAG1 + LAG2):
        if t >= LAG1 + LAG2:
            back(t - LAG1 - LAG2)
        if t < n:
            front(t)
        if 0 <= t - LAG1 < n:
            middle(t - LAG1)


def low(v, n):
    return lax.bitwise_and(v, jnp.int32(n - 1))


def high(v, bits):
    return lax.shift_right_logical(v, jnp.int32(bits))


def shift_of(s):
    r, x, core = high(s, 3), high(low(s, 8), 1), low(s, 2)
    return dealt_from(low(x + r + 2 * core, 4))


def dealt_from(m):
    return jnp.where(m == 0, 0, jnp.where(m == 1, -1, jnp.where(m == 2, 1, 0)))


def kernel(x_hbm, wf0, wf1, wg0, wg1, wres, wskip, hout, sout, x, w0, w1, w2, w3, w4, w5, w1t, wrt, wst, xbuf,
           hA, hB, hC, sA, sB, sC, aA, aB, aC, uA, uB, uC, hist, hstage, sstage,
           load_sem, in_send, in_recv, halo_send, out_send, out_recv):
    loads = [pltpu.make_async_copy(a, b, load_sem.at[i])
             for i, (a, b) in enumerate(zip((x_hbm, wf0, wf1, wg0, wg1, wres, wskip), (x, w0, w1, w2, w3, w4, w5)))]
    for load in loads:
        load.start()
    hi, k = lax.axis_index("seq_hi"), lax.axis_index("seq")
    z, row = high(hi, 2), low(hi, 4)
    me = row * 8 + k
    first = low(4 * z + shift_of(me), 16)

    def device(h, m):
        return {"seq_hi": h, "seq": m}

    def place(s):
        return dealt(shift_of(s))

    def dealt(off):
        e = low(hi - off, 16)
        q, c = high(e, 2), low(e, 4)
        return q, c, jnp.logical_and(c >= 1, low(4 * q + 4 + off, 16) + c >= 4)

    my_q, my_c, my_halo = place(me)
    keeps = my_q == z
    reuses = jnp.logical_and(my_halo, low(my_q + 1, 4) == z)
    mine = jnp.where(keeps, (3 + my_c) * NT + k, jnp.where(reuses, (my_c - 1) * NT + k, -1))

    def own_copy(s):
        q, c, _ = place(s)
        slot = (3 + c) * NT + k
        return pltpu.make_async_remote_copy(
            src_ref=x.at[s], dst_ref=xbuf.at[slot], send_sem=in_send.at[s], recv_sem=in_recv.at[slot],
            device_id=device(q * 4 + high(s, 3), low(s, 8)), device_id_type=MESH)

    def owns(s):
        return jnp.logical_or(s != me, jnp.logical_not(keeps))

    def halo_copy(s):
        q, c, _ = place(s)
        slot = (c - 1) * NT + k
        return pltpu.make_async_remote_copy(
            src_ref=x.at[s], dst_ref=xbuf.at[slot], send_sem=halo_send.at[s], recv_sem=in_recv.at[slot],
            device_id=device(low(q + 1, 4) * 4 + high(s, 3), low(s, 8)), device_id_type=MESH)

    def halos(s):
        return jnp.logical_and(place(s)[2], jnp.logical_or(s != me, jnp.logical_not(reuses)))

    def out_copy(i, src, dst, t):
        g = low(first + high(t, 3), 16)
        return pltpu.make_async_remote_copy(
            src_ref=src.at[t], dst_ref=dst.at[me], send_sem=out_send.at[i, t], recv_sem=out_recv.at[i, me],
            device_id=device(g, low(t, NT)), device_id_type=MESH)

    def leaves(t):
        return t + 3 * NT != mine

    barrier = pltpu.get_barrier_semaphore()

    def greet(i, c):
        for kk in range(7):
            g = first - 3 + kk

            @pl.when(jnp.logical_and(g >= 0, kk * NT + i != mine))
            def _():
                pl.semaphore_signal(barrier, inc=1, device_id=device(low(g, 16), i), device_id_type=MESH)
        return c

    lax.fori_loop(0, NT, greet, 0)
    peers = 32 - keeps.astype(jnp.int32) - reuses.astype(jnp.int32)
    for m in range(4):
        for parity in range(2):
            peers = peers + 4 * dealt(dealt_from(jnp.int32(m)))[2].astype(jnp.int32)
    loads[0].wait()
    pl.semaphore_wait(barrier, peers)

    def spread(body):
        core = low(k, 2)
        start = row + high(k, 1) + 2 * core

        def turn(i, carry):
            m = low(start + i, 4)
            for parity in range(2):
                q, c, halo = dealt(dealt_from(m))
                for j in range(4):
                    r, co = low(row + parity + 2 * (j // 2), 4), low(core + j, 2)
                    s = r * 8 + 2 * low(m - r - 2 * co, 4) + co
                    body(s, q, c, halo, r)
            return carry

        lax.fori_loop(0, 4, turn, 0)

    def start_halo(s, q, c, halo, r):
        @pl.when(jnp.logical_and(halo, jnp.logical_or(s != me, jnp.logical_not(reuses))))
        def _():
            slot = (c - 1) * NT + k
            pltpu.make_async_remote_copy(
                src_ref=x.at[s], dst_ref=xbuf.at[slot], send_sem=halo_send.at[s], recv_sem=in_recv.at[slot],
                device_id=device(low(q + 1, 4) * 4 + r, low(s, 8)), device_id_type=MESH).start()

    def start_own(s, q, c, halo, r):
        @pl.when(owns(s))
        def _():
            slot = (3 + c) * NT + k
            pltpu.make_async_remote_copy(
                src_ref=x.at[s], dst_ref=xbuf.at[slot], send_sem=in_send.at[s], recv_sem=in_recv.at[slot],
                device_id=device(q * 4 + r, low(s, 8)), device_id_type=MESH).start()

    spread(start_halo)
    spread(start_own)

    for load in loads[1:]:
        load.wait()

    def prepare(c, carry):
        for r in range(3):
            layer = r * CYCLE + c
            top = jnp.concatenate([w1[r, c], w3[r, c]], 1)
            bottom = jnp.concatenate([w0[r, c], w2[r, c]], 1)
            w1t[layer] = jnp.concatenate([top, bottom], 0).astype(F32).T.astype(BF)
            last = jnp.concatenate([w4[r, c], w5[r, c]], 1).astype(F32).T.astype(BF)
            wrt[layer] = last[:CHANS]
            wst[layer] = last[CHANS:]
        return carry

    lax.fori_loop(0, CYCLE, prepare, 0)

    lane = lax.broadcasted_iota(jnp.int32, (CHANS, TILE), 1)
    hist[...] = jnp.zeros_like(hist)

    @pl.when(mine >= 0)
    def _():
        xbuf[jnp.maximum(mine, 0)] = x[me]

    for kk in range(3):
        @pl.when(first - 3 + kk < 0)
        def _():
            xbuf[kk * NT : (kk + 1) * NT] = jnp.zeros((NT, CHANS, TILE), BF)

    def wait_chunk(kk):
        @pl.when(first - 3 + kk >= 0)
        def _():
            def wait_slot(slot, c):
                @pl.when(slot != mine)
                def _():
                    pltpu.make_async_copy(xbuf.at[slot], xbuf.at[slot], in_recv.at[slot]).wait()
                return c

            lax.fori_loop(kk * NT, kk * NT + NT, wait_slot, 0)

    for kk in range(3):
        wait_chunk(kk)

    def macro(s):
        @pl.when(s >= 3)
        def _():
            hC[...] = hB[...]
            sC[...] = sB[...]

        @pl.when(s >= 2)
        def _():
            hB[...] = hA[...]
            sB[...] = sA[...]

        @pl.when(s == 0)
        def _():
            hA[...] = xbuf[0:8].astype(F32)
            hB[...] = xbuf[8:16].astype(F32)
            hC[...] = xbuf[16:24].astype(F32)
            for ref in (sA, sB, sC):
                ref[...] = jnp.zeros_like(ref)

        @pl.when(jnp.logical_and(s >= 1, s <= 4))
        def _():
            wait_chunk(s + 2)
            hA[...] = xbuf[pl.ds((s + 2) * NT, NT)].astype(F32)
            sA[...] = jnp.zeros_like(sA)

        reps = [0, jnp.minimum(s, 1), jnp.minimum(s, 2)]
        resets = [first - 3 + s + i == 16 for i in (2, 1, 0)]
        run_layers(reps, resets, [hA, hB, hC], [sA, sB, sC], [aA, aB, aC], [uA, uB, uC], hist, w1t, wrt, wst, lane)

        @pl.when(s >= 3)
        def _():
            base = (s - 3) * NT
            hstage[pl.ds(base, NT)] = hC[...]
            sstage[pl.ds(base, NT)] = sC[...]

            def send(o, c):
                t = base + low(5 * o + k, NT)

                @pl.when(leaves(t))
                def _():
                    out_copy(0, hstage, hout, t).start()
                    out_copy(1, sstage, sout, t).start()
                return c

            lax.fori_loop(0, NT, send, 0)

    lax.fori_loop(0, 7, lambda s, c: (macro(s), c)[1], 0)

    @pl.when(keeps)
    def _():
        hout[me] = hstage[jnp.maximum(mine - 3 * NT, 0)]
        sout[me] = sstage[jnp.maximum(mine - 3 * NT, 0)]

    def drain_sends(s, c):
        @pl.when(owns(s))
        def _():
            own_copy(s).wait_send()

        @pl.when(halos(s))
        def _():
            halo_copy(s).wait_send()

        @pl.when(leaves(s))
        def _():
            out_copy(0, hstage, hout, s).wait_send()
            out_copy(1, sstage, sout, s).wait_send()
        return c

    lax.fori_loop(0, 32, drain_sends, 0)

    def drain(s, c):
        @pl.when(owns(s))
        def _():
            pltpu.make_async_copy(hout.at[s], hout.at[s], out_recv.at[0, s]).wait()
            pltpu.make_async_copy(sout.at[s], sout.at[s], out_recv.at[1, s]).wait()
        return c

    lax.fori_loop(0, 32, drain, 0)


def solution(mesh):
    seq_spec = P("batch", SEQ_AXES, None)

    def local_stack(x_loc, *weights):
        x_t = jnp.swapaxes(x_loc, 1, 2)
        V, D = pltpu.VMEM, pltpu.SemaphoreType.DMA
        hid = (NT, CHANS, TILE)
        out = jax.ShapeDtypeStruct((32, CHANS, TILE), F32)
        h, skip = pl.pallas_call(
            kernel,
            out_shape=[out, out],
            in_specs=[pl.BlockSpec(memory_space=pltpu.HBM)] * 7,
            out_specs=[pl.BlockSpec(memory_space=V)] * 2,
            scratch_shapes=[V((32, CHANS, TILE), BF)] + [V((3, CYCLE, CHANS, CHANS), BF)] * 6
            + [V((30, 2 * CHANS, 2 * CHANS), BF)] + [V((30, CHANS, CHANS), BF)] * 2
            + [V((56, CHANS, TILE), BF)] + [V(hid, F32)] * 6 + [V((4 * CHANS, NT * TILE), BF)] * 3
            + [V((NT + 4, CHANS, TILE), BF)] * 3 + [V((31, 4, CHANS, TILE), BF)] + [V((32, CHANS, TILE), F32)] * 2
            + [D((7,)), D((32,)), D((56,)), D((32,)), D((2, 32)), D((2, 32))],
            compiler_params=pltpu.CompilerParams(vmem_limit_bytes=24 * 2**20, has_side_effects=True, collective_id=0),
        )(*[pltpu.with_memory_space_constraint(a, pltpu.HBM) for a in (x_t, *weights)])
        return jnp.swapaxes(h, 1, 2), jnp.swapaxes(skip, 1, 2)

    return jax.shard_map(local_stack, mesh=mesh, in_specs=(seq_spec, P(), P(), P(), P(), P(), P()), out_specs=(seq_spec, seq_spec), check_vma=False)
```

```python
import jax
import jax.numpy as jnp
from jax import lax
from jax.experimental import pallas as pl
from jax.experimental.pallas import tpu as pltpu
from jax.sharding import PartitionSpec as P

F32, BF = jnp.float32, jnp.bfloat16
SEQ_AXES = ("seq_hi", "seq")
MESH = pl.DeviceIdType.MESH
NT = 8
HALO = 24
LAG1, LAG2 = 5, 4
ZERO = 30
CHANS, TILE, CYCLE = 64, 128, 10


def run_layers(reps, resets, hs, ss, acts, us, hist, w1t, wrt, wst, lane):
    items = [(c, st, j) for c in range(CYCLE) for st in range(len(reps)) for j in range(0, NT, 2)]
    carry, gates, mixed, skips = {}, {}, {}, {}

    def front(t):
        c, st, j = items[t]
        d = 2**c
        nh = max(1, d // TILE)
        layer = reps[st] * CYCLE + c
        h, ub = hs[st], us[st]
        if j == 0:
            for i in range(4 - nh, 4):
                ub[i] = hist[jnp.where(resets[st], ZERO, layer), i]
            if d < TILE:
                carry[st] = pltpu.roll(ub[3], d, 1)
        u = [h[j].astype(BF), h[j + 1].astype(BF)]
        if d >= TILE:
            ub[4 + j], ub[5 + j] = u[0], u[1]
            q = d // TILE
            p = [ub[4 + j - q], ub[5 + j - q] if q > 1 else u[0]]
        else:
            r0, r1 = pltpu.roll(u[0], d, 1), pltpu.roll(u[1], d, 1)
            p = [jnp.where(lane < d, carry[st], r0), jnp.where(lane < d, r0, r1)]
            carry[st] = r1
        for i in range(2):
            k = j + i - (NT - 4)
            if k >= 4 - nh:
                hist[layer, k] = u[i]
        up = jnp.concatenate([jnp.concatenate(u, 1), jnp.concatenate(p, 1)], 0)
        gates[t] = jnp.dot(w1t[layer], up, preferred_element_type=F32)

    def middle(t):
        c, st, j = items[t]
        layer = reps[st] * CYCLE + c
        g = gates.pop(t)
        sig = jnp.tanh(g[CHANS:] * 0.5) * 0.5 + 0.5
        a = (jnp.tanh(g[:CHANS]) * sig).astype(BF)
        row = (c % 4) * CHANS
        cols = slice(j * TILE, (j + 2) * TILE)
        if c not in (3, 7, 9):
            acts[st][row : row + CHANS, cols] = a
        mixed[t] = jnp.dot(wrt[layer], a, preferred_element_type=F32)
        if c in (3, 7, 9):
            stack = jnp.concatenate([acts[st][:row, cols], a], 0)
            ws = jnp.concatenate([wst[layer - c % 4 + i] for i in range(c % 4 + 1)], 1)
            skips[t] = jnp.dot(ws, stack, preferred_element_type=F32)

    def back(t):
        c, st, j = items[t]
        res = mixed.pop(t)
        h = hs[st]
        h[j] += res[:, :TILE]
        h[j + 1] += res[:, TILE:]
        if t in skips:
            res = skips.pop(t)
            ss[st][j] += res[:, :TILE]
            ss[st][j + 1] += res[:, TILE:]

    n = len(items)
    for t in range(n + LAG1 + LAG2):
        if t >= LAG1 + LAG2:
            back(t - LAG1 - LAG2)
        if t < n:
            front(t)
        if 0 <= t - LAG1 < n:
            middle(t - LAG1)


def low(v, n):
    return lax.bitwise_and(v, jnp.int32(n - 1))


def high(v, bits):
    return lax.shift_right_logical(v, jnp.int32(bits))


def shift_of(s):
    r, x, core = high(s, 3), high(low(s, 8), 1), low(s, 2)
    return dealt_from(low(x + r + 2 * core, 4))


def dealt_from(m):
    return jnp.where(m == 0, 0, jnp.where(m == 1, -1, jnp.where(m == 2, 1, 0)))


def kernel(x_hbm, wf0, wf1, wg0, wg1, wres, wskip, hout, sout, x, w0, w1, w2, w3, w4, w5, w1t, wrt, wst, xbuf,
           hA, hB, hC, sA, sB, sC, aA, aB, aC, uA, uB, uC, hist, hstage, sstage,
           load_sem, in_send, in_recv, halo_send, out_send, out_recv):
    loads = [pltpu.make_async_copy(a, b, load_sem.at[i])
             for i, (a, b) in enumerate(zip((x_hbm, wf0, wf1, wg0, wg1, wres, wskip), (x, w0, w1, w2, w3, w4, w5)))]
    for load in loads:
        load.start()
    hi, k = lax.axis_index("seq_hi"), lax.axis_index("seq")
    z, row = high(hi, 2), low(hi, 4)
    me = row * 8 + k
    first = low(4 * z + shift_of(me), 16)

    def device(h, m):
        return {"seq_hi": h, "seq": m}

    def place(s):
        return dealt(shift_of(s))

    def dealt(off):
        e = low(hi - off, 16)
        q, c = high(e, 2), low(e, 4)
        return q, c, jnp.logical_and(c >= 1, low(4 * q + 4 + off, 16) + c >= 4)

    my_q, my_c, my_halo = place(me)
    keeps = my_q == z
    reuses = jnp.logical_and(my_halo, low(my_q + 1, 4) == z)
    mine = jnp.where(keeps, (3 + my_c) * NT + k, jnp.where(reuses, (my_c - 1) * NT + k, -1))

    def own_copy(s):
        q, c, _ = place(s)
        slot = (3 + c) * NT + k
        return pltpu.make_async_remote_copy(
            src_ref=x.at[s], dst_ref=xbuf.at[slot], send_sem=in_send.at[s], recv_sem=in_recv.at[slot],
            device_id=device(q * 4 + high(s, 3), low(s, 8)), device_id_type=MESH)

    def owns(s):
        return jnp.logical_or(s != me, jnp.logical_not(keeps))

    def halo_copy(s):
        q, c, _ = place(s)
        slot = (c - 1) * NT + k
        return pltpu.make_async_remote_copy(
            src_ref=x.at[s], dst_ref=xbuf.at[slot], send_sem=halo_send.at[s], recv_sem=in_recv.at[slot],
            device_id=device(low(q + 1, 4) * 4 + high(s, 3), low(s, 8)), device_id_type=MESH)

    def halos(s):
        return jnp.logical_and(place(s)[2], jnp.logical_or(s != me, jnp.logical_not(reuses)))

    def out_copy(i, src, dst, t):
        g = low(first + high(t, 3), 16)
        return pltpu.make_async_remote_copy(
            src_ref=src.at[t], dst_ref=dst.at[me], send_sem=out_send.at[i, t], recv_sem=out_recv.at[i, me],
            device_id=device(g, low(t, NT)), device_id_type=MESH)

    def leaves(t):
        return t + 3 * NT != mine

    barrier = pltpu.get_barrier_semaphore()

    def greet(i, c):
        for kk in range(7):
            g = first - 3 + kk

            @pl.when(jnp.logical_and(g >= 0, kk * NT + i != mine))
            def _():
                pl.semaphore_signal(barrier, inc=1, device_id=device(low(g, 16), i), device_id_type=MESH)
        return c

    lax.fori_loop(0, NT, greet, 0)
    peers = 32 - keeps.astype(jnp.int32) - reuses.astype(jnp.int32)
    for m in range(4):
        for parity in range(2):
            peers = peers + 4 * dealt(dealt_from(jnp.int32(m)))[2].astype(jnp.int32)
    loads[0].wait()
    pl.semaphore_wait(barrier, peers)

    def spread(body):
        core = low(k, 2)
        start = row + high(k, 1) + 2 * core

        def turn(i, carry):
            m = low(start + i, 4)
            for parity in range(2):
                q, c, halo = dealt(dealt_from(m))
                for j in range(4):
                    r, co = low(row + parity + 2 * (j // 2), 4), low(core + j, 2)
                    s = r * 8 + 2 * low(m - r - 2 * co, 4) + co
                    body(s, q, c, halo, r)
            return carry

        lax.fori_loop(0, 4, turn, 0)

    def start_halo(s, q, c, halo, r):
        @pl.when(jnp.logical_and(halo, jnp.logical_or(s != me, jnp.logical_not(reuses))))
        def _():
            slot = (c - 1) * NT + k
            pltpu.make_async_remote_copy(
                src_ref=x.at[s], dst_ref=xbuf.at[slot], send_sem=halo_send.at[s], recv_sem=in_recv.at[slot],
                device_id=device(low(q + 1, 4) * 4 + r, low(s, 8)), device_id_type=MESH).start()

    def start_own(s, q, c, halo, r):
        @pl.when(owns(s))
        def _():
            slot = (3 + c) * NT + k
            pltpu.make_async_remote_copy(
                src_ref=x.at[s], dst_ref=xbuf.at[slot], send_sem=in_send.at[s], recv_sem=in_recv.at[slot],
                device_id=device(q * 4 + r, low(s, 8)), device_id_type=MESH).start()

    spread(start_halo)
    spread(start_own)

    for load in loads[1:]:
        load.wait()

    def prepare(c, carry):
        for r in range(3):
            layer = r * CYCLE + c
            top = jnp.concatenate([w1[r, c], w3[r, c]], 1)
            bottom = jnp.concatenate([w0[r, c], w2[r, c]], 1)
            w1t[layer] = jnp.concatenate([top, bottom], 0).astype(F32).T.astype(BF)
            last = jnp.concatenate([w4[r, c], w5[r, c]], 1).astype(F32).T.astype(BF)
            wrt[layer] = last[:CHANS]
            wst[layer] = last[CHANS:]
        return carry

    lax.fori_loop(0, CYCLE, prepare, 0)

    lane = lax.broadcasted_iota(jnp.int32, (CHANS, TILE), 1)
    hist[...] = jnp.zeros_like(hist)

    @pl.when(mine >= 0)
    def _():
        xbuf[jnp.maximum(mine, 0)] = x[me]

    for kk in range(3):
        @pl.when(first - 3 + kk < 0)
        def _():
            xbuf[kk * NT : (kk + 1) * NT] = jnp.zeros((NT, CHANS, TILE), BF)

    def wait_chunk(kk):
        @pl.when(first - 3 + kk >= 0)
        def _():
            def wait_slot(slot, c):
                @pl.when(slot != mine)
                def _():
                    pltpu.make_async_copy(xbuf.at[slot], xbuf.at[slot], in_recv.at[slot]).wait()
                return c

            lax.fori_loop(kk * NT, kk * NT + NT, wait_slot, 0)

    for kk in range(3):
        wait_chunk(kk)

    def macro(s):
        @pl.when(s >= 3)
        def _():
            hC[...] = hB[...]
            sC[...] = sB[...]

        @pl.when(s >= 2)
        def _():
            hB[...] = hA[...]
            sB[...] = sA[...]

        @pl.when(s == 0)
        def _():
            hA[...] = xbuf[0:8].astype(F32)
            hB[...] = xbuf[8:16].astype(F32)
            hC[...] = xbuf[16:24].astype(F32)
            for ref in (sA, sB, sC):
                ref[...] = jnp.zeros_like(ref)

        @pl.when(jnp.logical_and(s >= 1, s <= 4))
        def _():
            wait_chunk(s + 2)
            hA[...] = xbuf[pl.ds((s + 2) * NT, NT)].astype(F32)
            sA[...] = jnp.zeros_like(sA)

        reps = [0, jnp.minimum(s, 1), jnp.minimum(s, 2)]
        resets = [first - 3 + s + i == 16 for i in (2, 1, 0)]
        run_layers(reps, resets, [hA, hB, hC], [sA, sB, sC], [aA, aB, aC], [uA, uB, uC], hist, w1t, wrt, wst, lane)

        @pl.when(s >= 3)
        def _():
            base = (s - 3) * NT
            hstage[pl.ds(base, NT)] = hC[...]
            sstage[pl.ds(base, NT)] = sC[...]

            def send(o, c):
                t = base + low(5 * o + k, NT)

                @pl.when(leaves(t))
                def _():
                    out_copy(0, hstage, hout, t).start()
                    out_copy(1, sstage, sout, t).start()
                return c

            lax.fori_loop(0, NT, send, 0)

    lax.fori_loop(0, 7, lambda s, c: (macro(s), c)[1], 0)

    @pl.when(keeps)
    def _():
        hout[me] = hstage[jnp.maximum(mine - 3 * NT, 0)]
        sout[me] = sstage[jnp.maximum(mine - 3 * NT, 0)]

    def drain_sends(s, c):
        @pl.when(owns(s))
        def _():
            own_copy(s).wait_send()

        @pl.when(halos(s))
        def _():
            halo_copy(s).wait_send()

        @pl.when(leaves(s))
        def _():
            out_copy(0, hstage, hout, s).wait_send()
            out_copy(1, sstage, sout, s).wait_send()
        return c

    lax.fori_loop(0, 32, drain_sends, 0)

    def drain(s, c):
        @pl.when(owns(s))
        def _():
            pltpu.make_async_copy(hout.at[s], hout.at[s], out_recv.at[0, s]).wait()
            pltpu.make_async_copy(sout.at[s], sout.at[s], out_recv.at[1, s]).wait()
        return c

    lax.fori_loop(0, 32, drain, 0)


def leave(h, skip, h_out, skip_out, sems):
    copies = [pltpu.make_async_copy(a.at[pl.ds(16 * i, 16)], b.at[pl.ds(16 * i, 16)], sems.at[i, n])
              for n, (a, b) in enumerate(((h, h_out), (skip, skip_out))) for i in range(2)]
    for copy in copies:
        copy.start()
    for copy in copies:
        copy.wait()


def solution(mesh):
    seq_spec = P("batch", SEQ_AXES, None)

    def local_stack(x_loc, *weights):
        x_t = jnp.swapaxes(x_loc, 1, 2)
        V, D = pltpu.VMEM, pltpu.SemaphoreType.DMA
        hid = (NT, CHANS, TILE)
        out = jax.ShapeDtypeStruct((32, CHANS, TILE), F32)
        h, skip = pl.pallas_call(
            kernel,
            out_shape=[out, out],
            in_specs=[pl.BlockSpec(memory_space=pltpu.HBM)] * 7,
            out_specs=[pl.BlockSpec(memory_space=V)] * 2,
            scratch_shapes=[V((32, CHANS, TILE), BF)] + [V((3, CYCLE, CHANS, CHANS), BF)] * 6
            + [V((30, 2 * CHANS, 2 * CHANS), BF)] + [V((30, CHANS, CHANS), BF)] * 2
            + [V((56, CHANS, TILE), BF)] + [V(hid, F32)] * 6 + [V((4 * CHANS, NT * TILE), BF)] * 3
            + [V((NT + 4, CHANS, TILE), BF)] * 3 + [V((31, 4, CHANS, TILE), BF)] + [V((32, CHANS, TILE), F32)] * 2
            + [D((7,)), D((32,)), D((56,)), D((32,)), D((2, 32)), D((2, 32))],
            compiler_params=pltpu.CompilerParams(vmem_limit_bytes=24 * 2**20, has_side_effects=True, collective_id=0),
        )(*[pltpu.with_memory_space_constraint(a, pltpu.HBM) for a in (x_t, *weights)])
        h, skip = pl.pallas_call(
            leave,
            out_shape=[out, out],
            in_specs=[pl.BlockSpec(memory_space=V)] * 2,
            out_specs=[pl.BlockSpec(memory_space=pltpu.HBM)] * 2,
            scratch_shapes=[D((2, 2))],
            compiler_params=pltpu.CompilerParams(vmem_limit_bytes=8 * 2**20),
        )(h, skip)
        return jnp.swapaxes(h, 1, 2), jnp.swapaxes(skip, 1, 2)

    return jax.shard_map(local_stack, mesh=mesh, in_specs=(seq_spec, P(), P(), P(), P(), P(), P()), out_specs=(seq_spec, seq_spec), check_vma=False)
```

```python
import jax
import jax.numpy as jnp
from jax import lax
from jax.experimental import pallas as pl
from jax.experimental.pallas import tpu as pltpu
from jax.sharding import PartitionSpec as P

F32, BF = jnp.float32, jnp.bfloat16
SEQ_AXES = ("seq_hi", "seq")
MESH = pl.DeviceIdType.MESH
NT = 8
HALO = 24
LAG1, LAG2 = 5, 4
ZERO = 30
CHANS, TILE, CYCLE = 64, 128, 10


def run_layers(reps, resets, hs, ss, acts, us, hist, w1t, wrt, wst, lane):
    items = [(c, st, j) for c in range(CYCLE) for st in range(len(reps)) for j in range(0, NT, 2)]
    carry, gates, mixed, skips = {}, {}, {}, {}

    def front(t):
        c, st, j = items[t]
        d = 2**c
        nh = max(1, d // TILE)
        layer = reps[st] * CYCLE + c
        h, ub = hs[st], us[st]
        if j == 0:
            for i in range(4 - nh, 4):
                ub[i] = hist[jnp.where(resets[st], ZERO, layer), i]
            if d < TILE:
                carry[st] = pltpu.roll(ub[3], d, 1)
        u = [h[j].astype(BF), h[j + 1].astype(BF)]
        if d >= TILE:
            ub[4 + j], ub[5 + j] = u[0], u[1]
            q = d // TILE
            p = [ub[4 + j - q], ub[5 + j - q] if q > 1 else u[0]]
        else:
            r0, r1 = pltpu.roll(u[0], d, 1), pltpu.roll(u[1], d, 1)
            p = [jnp.where(lane < d, carry[st], r0), jnp.where(lane < d, r0, r1)]
            carry[st] = r1
        for i in range(2):
            k = j + i - (NT - 4)
            if k >= 4 - nh:
                hist[layer, k] = u[i]
        up = jnp.concatenate([jnp.concatenate(u, 1), jnp.concatenate(p, 1)], 0)
        gates[t] = jnp.dot(w1t[layer], up, preferred_element_type=F32)

    def middle(t):
        c, st, j = items[t]
        layer = reps[st] * CYCLE + c
        g = gates.pop(t)
        sig = jnp.tanh(g[CHANS:] * 0.5) * 0.5 + 0.5
        a = (jnp.tanh(g[:CHANS]) * sig).astype(BF)
        row = (c % 4) * CHANS
        cols = slice(j * TILE, (j + 2) * TILE)
        if c not in (3, 7, 9):
            acts[st][row : row + CHANS, cols] = a
        mixed[t] = jnp.dot(wrt[layer], a, preferred_element_type=F32)
        if c in (3, 7, 9):
            stack = jnp.concatenate([acts[st][:row, cols], a], 0)
            ws = jnp.concatenate([wst[layer - c % 4 + i] for i in range(c % 4 + 1)], 1)
            skips[t] = jnp.dot(ws, stack, preferred_element_type=F32)

    def back(t):
        c, st, j = items[t]
        res = mixed.pop(t)
        h = hs[st]
        h[j] += res[:, :TILE]
        h[j + 1] += res[:, TILE:]
        if t in skips:
            res = skips.pop(t)
            ss[st][j] += res[:, :TILE]
            ss[st][j + 1] += res[:, TILE:]

    n = len(items)
    for t in range(n + LAG1 + LAG2):
        if t >= LAG1 + LAG2:
            back(t - LAG1 - LAG2)
        if t < n:
            front(t)
        if 0 <= t - LAG1 < n:
            middle(t - LAG1)


def low(v, n):
    return lax.bitwise_and(v, jnp.int32(n - 1))


def high(v, bits):
    return lax.shift_right_logical(v, jnp.int32(bits))


def shift_of(s):
    r, x, core = high(s, 3), high(low(s, 8), 1), low(s, 2)
    return dealt_from(low(x + r + 2 * core, 4))


def dealt_from(m):
    return jnp.where(m == 0, 0, jnp.where(m == 1, -1, jnp.where(m == 2, 1, 0)))


def kernel(x_hbm, wf0, wf1, wg0, wg1, wres, wskip, hout, sout, x, w0, w1, w2, w3, w4, w5, w1t, wrt, wst, xbuf,
           hA, hB, hC, sA, sB, sC, aA, aB, aC, uA, uB, uC, hist, hstage, sstage,
           load_sem, in_send, in_recv, halo_send, out_send, out_recv):
    loads = [pltpu.make_async_copy(a, b, load_sem.at[i])
             for i, (a, b) in enumerate(zip((x_hbm, wf0, wf1, wg0, wg1, wres, wskip), (x, w0, w1, w2, w3, w4, w5)))]
    for load in loads:
        load.start()
    hi, k = lax.axis_index("seq_hi"), lax.axis_index("seq")
    z, row = high(hi, 2), low(hi, 4)
    me = row * 8 + k
    first = low(4 * z + shift_of(me), 16)

    def device(h, m):
        return {"seq_hi": h, "seq": m}

    def place(s):
        return dealt(shift_of(s))

    def dealt(off):
        e = low(hi - off, 16)
        q, c = high(e, 2), low(e, 4)
        return q, c, jnp.logical_and(c >= 1, low(4 * q + 4 + off, 16) + c >= 4)

    my_q, my_c, my_halo = place(me)
    keeps = my_q == z
    reuses = jnp.logical_and(my_halo, low(my_q + 1, 4) == z)
    mine = jnp.where(keeps, (3 + my_c) * NT + k, jnp.where(reuses, (my_c - 1) * NT + k, -1))

    def own_copy(s):
        q, c, _ = place(s)
        slot = (3 + c) * NT + k
        return pltpu.make_async_remote_copy(
            src_ref=x.at[s], dst_ref=xbuf.at[slot], send_sem=in_send.at[s], recv_sem=in_recv.at[slot],
            device_id=device(q * 4 + high(s, 3), low(s, 8)), device_id_type=MESH)

    def owns(s):
        return jnp.logical_or(s != me, jnp.logical_not(keeps))

    def halo_copy(s):
        q, c, _ = place(s)
        slot = (c - 1) * NT + k
        return pltpu.make_async_remote_copy(
            src_ref=x.at[s], dst_ref=xbuf.at[slot], send_sem=halo_send.at[s], recv_sem=in_recv.at[slot],
            device_id=device(low(q + 1, 4) * 4 + high(s, 3), low(s, 8)), device_id_type=MESH)

    def halos(s):
        return jnp.logical_and(place(s)[2], jnp.logical_or(s != me, jnp.logical_not(reuses)))

    def out_copy(i, src, dst, t):
        g = low(first + high(t, 3), 16)
        return pltpu.make_async_remote_copy(
            src_ref=src.at[t], dst_ref=dst.at[me], send_sem=out_send.at[i, t], recv_sem=out_recv.at[i, me],
            device_id=device(g, low(t, NT)), device_id_type=MESH)

    def leaves(t):
        return t + 3 * NT != mine

    barrier = pltpu.get_barrier_semaphore()

    def greet(i, c):
        for kk in range(7):
            g = first - 3 + kk

            @pl.when(jnp.logical_and(g >= 0, kk * NT + i != mine))
            def _():
                pl.semaphore_signal(barrier, inc=1, device_id=device(low(g, 16), i), device_id_type=MESH)
        return c

    lax.fori_loop(0, NT, greet, 0)
    peers = 32 - keeps.astype(jnp.int32) - reuses.astype(jnp.int32)
    for m in range(4):
        for parity in range(2):
            peers = peers + 4 * dealt(dealt_from(jnp.int32(m)))[2].astype(jnp.int32)
    loads[0].wait()
    pl.semaphore_wait(barrier, peers)

    def spread(body):
        core = low(k, 2)
        start = row + high(k, 1) + 2 * core

        def turn(i, carry):
            m = low(start + i, 4)
            for parity in range(2):
                q, c, halo = dealt(dealt_from(m))
                for j in range(4):
                    r, co = low(row + parity + 2 * (j // 2), 4), low(core + j, 2)
                    s = r * 8 + 2 * low(m - r - 2 * co, 4) + co
                    body(s, q, c, halo, r)
            return carry

        lax.fori_loop(0, 4, turn, 0)

    def start_halo(s, q, c, halo, r):
        @pl.when(jnp.logical_and(halo, jnp.logical_or(s != me, jnp.logical_not(reuses))))
        def _():
            slot = (c - 1) * NT + k
            pltpu.make_async_remote_copy(
                src_ref=x.at[s], dst_ref=xbuf.at[slot], send_sem=halo_send.at[s], recv_sem=in_recv.at[slot],
                device_id=device(low(q + 1, 4) * 4 + r, low(s, 8)), device_id_type=MESH).start()

    def start_own(s, q, c, halo, r):
        @pl.when(owns(s))
        def _():
            slot = (3 + c) * NT + k
            pltpu.make_async_remote_copy(
                src_ref=x.at[s], dst_ref=xbuf.at[slot], send_sem=in_send.at[s], recv_sem=in_recv.at[slot],
                device_id=device(q * 4 + r, low(s, 8)), device_id_type=MESH).start()

    spread(start_halo)
    spread(start_own)

    for load in loads[1:]:
        load.wait()

    def prepare(c, carry):
        for r in range(3):
            layer = r * CYCLE + c
            top = jnp.concatenate([w1[r, c], w3[r, c]], 1)
            bottom = jnp.concatenate([w0[r, c], w2[r, c]], 1)
            w1t[layer] = jnp.concatenate([top, bottom], 0).astype(F32).T.astype(BF)
            last = jnp.concatenate([w4[r, c], w5[r, c]], 1).astype(F32).T.astype(BF)
            wrt[layer] = last[:CHANS]
            wst[layer] = last[CHANS:]
        return carry

    lax.fori_loop(0, CYCLE, prepare, 0)

    lane = lax.broadcasted_iota(jnp.int32, (CHANS, TILE), 1)
    for ref in (hist, sA, sB, sC):
        ref[...] = jnp.zeros_like(ref)

    @pl.when(mine >= 0)
    def _():
        xbuf[jnp.maximum(mine, 0)] = x[me]

    for kk in range(3):
        @pl.when(first - 3 + kk < 0)
        def _():
            xbuf[kk * NT : (kk + 1) * NT] = jnp.zeros((NT, CHANS, TILE), BF)

    def wait_chunk(kk):
        @pl.when(first - 3 + kk >= 0)
        def _():
            def wait_slot(slot, c):
                @pl.when(slot != mine)
                def _():
                    pltpu.make_async_copy(xbuf.at[slot], xbuf.at[slot], in_recv.at[slot]).wait()
                return c

            lax.fori_loop(kk * NT, kk * NT + NT, wait_slot, 0)

    for kk in range(3):
        wait_chunk(kk)

    def macro(s):
        @pl.when(s >= 3)
        def _():
            hC[...] = hB[...]
            sC[...] = sB[...]

        @pl.when(s >= 2)
        def _():
            hB[...] = hA[...]
            sB[...] = sA[...]

        @pl.when(s == 0)
        def _():
            hA[...] = xbuf[0:8].astype(F32)
            hB[...] = xbuf[8:16].astype(F32)
            hC[...] = xbuf[16:24].astype(F32)

        @pl.when(jnp.logical_and(s >= 1, s <= 4))
        def _():
            wait_chunk(s + 2)
            hA[...] = xbuf[pl.ds((s + 2) * NT, NT)].astype(F32)
            sA[...] = jnp.zeros_like(sA)

        reps = [0, jnp.minimum(s, 1), jnp.minimum(s, 2)]
        resets = [first - 3 + s + i == 16 for i in (2, 1, 0)]
        run_layers(reps, resets, [hA, hB, hC], [sA, sB, sC], [aA, aB, aC], [uA, uB, uC], hist, w1t, wrt, wst, lane)

        @pl.when(s >= 3)
        def _():
            base = (s - 3) * NT
            hstage[pl.ds(base, NT)] = hC[...]
            sstage[pl.ds(base, NT)] = sC[...]

            def send(o, c):
                t = base + low(k + 2 * o + high(o, 2), NT)

                @pl.when(leaves(t))
                def _():
                    out_copy(0, hstage, hout, t).start()
                    out_copy(1, sstage, sout, t).start()
                return c

            lax.fori_loop(0, NT, send, 0)

    lax.fori_loop(0, 7, lambda s, c: (macro(s), c)[1], 0)

    @pl.when(keeps)
    def _():
        hout[me] = hstage[jnp.maximum(mine - 3 * NT, 0)]
        sout[me] = sstage[jnp.maximum(mine - 3 * NT, 0)]

    def drain_sends(s, c):
        @pl.when(owns(s))
        def _():
            own_copy(s).wait_send()

        @pl.when(halos(s))
        def _():
            halo_copy(s).wait_send()

        @pl.when(leaves(s))
        def _():
            out_copy(0, hstage, hout, s).wait_send()
            out_copy(1, sstage, sout, s).wait_send()
        return c

    lax.fori_loop(0, 32, drain_sends, 0)

    def drain(s, c):
        @pl.when(owns(s))
        def _():
            pltpu.make_async_copy(hout.at[s], hout.at[s], out_recv.at[0, s]).wait()
            pltpu.make_async_copy(sout.at[s], sout.at[s], out_recv.at[1, s]).wait()
        return c

    lax.fori_loop(0, 32, drain, 0)


def leave(h, skip, h_out, skip_out, sems):
    copies = [pltpu.make_async_copy(a.at[pl.ds(16 * i, 16)], b.at[pl.ds(16 * i, 16)], sems.at[i, n])
              for n, (a, b) in enumerate(((h, h_out), (skip, skip_out))) for i in range(2)]
    for copy in copies:
        copy.start()
    for copy in copies:
        copy.wait()


def solution(mesh):
    seq_spec = P("batch", SEQ_AXES, None)

    def local_stack(x_loc, *weights):
        x_t = jnp.swapaxes(x_loc, 1, 2)
        V, D = pltpu.VMEM, pltpu.SemaphoreType.DMA
        hid = (NT, CHANS, TILE)
        out = jax.ShapeDtypeStruct((32, CHANS, TILE), F32)
        h, skip = pl.pallas_call(
            kernel,
            out_shape=[out, out],
            in_specs=[pl.BlockSpec(memory_space=pltpu.HBM)] * 7,
            out_specs=[pl.BlockSpec(memory_space=V)] * 2,
            scratch_shapes=[V((32, CHANS, TILE), BF)] + [V((3, CYCLE, CHANS, CHANS), BF)] * 6
            + [V((30, 2 * CHANS, 2 * CHANS), BF)] + [V((30, CHANS, CHANS), BF)] * 2
            + [V((56, CHANS, TILE), BF)] + [V(hid, F32)] * 6 + [V((4 * CHANS, NT * TILE), BF)] * 3
            + [V((NT + 4, CHANS, TILE), BF)] * 3 + [V((31, 4, CHANS, TILE), BF)] + [V((32, CHANS, TILE), F32)] * 2
            + [D((7,)), D((32,)), D((56,)), D((32,)), D((2, 32)), D((2, 32))],
            compiler_params=pltpu.CompilerParams(vmem_limit_bytes=24 * 2**20, has_side_effects=True, collective_id=0),
        )(*[pltpu.with_memory_space_constraint(a, pltpu.HBM) for a in (x_t, *weights)])
        h, skip = pl.pallas_call(
            leave,
            out_shape=[out, out],
            in_specs=[pl.BlockSpec(memory_space=V)] * 2,
            out_specs=[pl.BlockSpec(memory_space=pltpu.HBM)] * 2,
            scratch_shapes=[D((2, 2))],
            compiler_params=pltpu.CompilerParams(vmem_limit_bytes=8 * 2**20),
        )(h, skip)
        return jnp.swapaxes(h, 1, 2), jnp.swapaxes(skip, 1, 2)

    return jax.shard_map(local_stack, mesh=mesh, in_specs=(seq_spec, P(), P(), P(), P(), P(), P()), out_specs=(seq_spec, seq_spec), check_vma=False)
```
